256 devices in a mesh: seq: 128 (over y, x, z), slide: 2 (over core).
Axes of the slice: x: 4, y: 4, z: 8, core: 2. Of those that a mesh axis runs over, the one named last changes fastest.
Arguments:
- tile_embed: bfloat16 [131072, 768], P(('slide', 'seq')), parts along dimension 0, may hold values from -6 to 6
- valid_tiles: int32 [2], P('slide'), parts along dimension 0, may hold values from 32768 to 65536
- offsets: int32 [16], replicated, may hold values from 0 to 15
- norm_gain: float32 [768], replicated, may hold values from 0.1 to 1.9
- w_qkv: bfloat16 [768, 2304], replicated
- sub_gain: float32 [768], replicated, may hold values from 0.1 to 1.9
- w_out: bfloat16 [768, 768], replicated, may hold values from -0.21875 to 0.21875
Outputs:
- encoded: bfloat16 [131072, 768], P(('slide', 'seq')), parts along dimension 0
The draws below stay inside these ranges and needn't reach their ends.
There are 2 independent parts, one for each index of `slide`. The reference program is written for one: setup_inputs(seed, part) draws one part's arguments, and reference() takes and returns one part's arrays. A program takes and returns all parts, laid end to end along the dimension named above; an argument that names none is the same for every part. Nothing has to cross between parts.
All inputs are finite; a program needn't handle non-finite values.
Results may differ from the reference program's by a relative error of at most 0.0078.
Values may be sent and summed in bfloat16 or wider, within the bound.
No kernel may reach another device: no remote copies, remote signals or barrier semaphores. Data moves between devices by JAX's collectives and lax.ppermute only.
A program may use at most 128 MiB of HBM per device.

```python
import jax
import jax.numpy as jnp
from jax import lax

D = 768
HEADS = 16
DEVICE_TOKENS = 512
SLIDE_TOKENS = 65536
NEAR_SPAN = 2
MIDDLE_DILATION = 4
FAR_DILATION = 16
MIDDLE_SPAN = 8
FAR_SEGMENT_SPAN = 32
N_SEQ = 128


def draw_w_qkv(key, part):
    key_query = jax.random.fold_in(key, 11)
    key_keys = jax.random.fold_in(key, 12)
    key_values = jax.random.fold_in(key, 13)
    spread_scale = D ** (-0.5)
    query_w = jax.random.normal(key_query, (D, D), jnp.float32) * spread_scale
    value_w = jax.random.normal(key_values, (D, D), jnp.float32) * spread_scale
    key_w = jax.random.normal(key_keys, (D, D), jnp.float32) * spread_scale
    return jnp.concatenate([query_w, key_w, value_w], axis=1).astype(jnp.bfloat16)


def with_ends(entries, key, least, high):
    extent = entries.shape
    spot = [jax.random.randint(jax.random.fold_in(key, axis), (), 0, extent[axis]) for axis in range(len(extent))]
    entries = entries.at[tuple(spot)].set(least)
    longest = extent.index(max(extent))
    spot[longest] = (spot[longest] + 1) % extent[longest]
    return entries.at[tuple(spot)].set(high)


def block_levels(own_key, extent, shards, low, top_value):
    def one(position, parts):
        steps = jax.random.uniform(jax.random.fold_in(jax.random.fold_in(own_key, 6), position), (parts,), jnp.float32, low / len(shards), top_value / len(shards))
        return jnp.repeat(jnp.exp(steps), extent[position] // parts).reshape((-1,) + (1,) * (len(extent) - position - 1))

    loudness = one(*shards[0])
    for cut in shards[1:]:
        loudness = loudness * one(*cut)
    return loudness


def noise(stream_key, dims, spread, bound, shards=(), kind=jnp.bfloat16):
    drawn = jax.random.normal(stream_key, dims, jnp.float32) * spread
    if len(shards) > 0:
        drawn = block_levels(stream_key, dims, shards, -0.22, 0.18) * drawn
    return jnp.clip(drawn, min=-bound, max=bound).astype(kind)


def setup_inputs(seed: int = 0, part: int = 0) -> dict:
    key_list = jax.random.split(jax.random.key(seed), 8)
    own_keys = jax.random.split(jax.random.fold_in(key_list[7], part), 8)
    return {
        "tile_embed": noise(own_keys[0], (SLIDE_TOKENS, D), 1.0, 6.0, ((0, 128),)),
        "valid_tiles": jax.random.randint(own_keys[1], (1,), SLIDE_TOKENS // 2, SLIDE_TOKENS + 1).astype(jnp.int32),
        "offsets": with_ends(jax.random.randint(key_list[2], (HEADS,), 0, 16), jax.random.fold_in(key_list[2], 1), 0, 15).astype(jnp.int32),
        "norm_gain": jnp.clip(1.0 + 0.18 * jax.random.normal(key_list[3], (D,), jnp.float32), 0.1, 1.9),
        "w_qkv": draw_w_qkv(jax.random.fold_in(key_list[7], 71), part),
        "sub_gain": jnp.clip(1.0 + 0.18 * jax.random.normal(key_list[5], (D,), jnp.float32), 0.1, 1.9),
        "w_out": noise(key_list[6], (D, D), D ** -0.5, 0.21875),
    }


NEGATIVE = -1e+30
EPSILON = 1e-05

def layer_norm(matrix, gain_row):
    average = lax.optimization_barrier(jnp.mean(matrix, axis=-1, keepdims=True))
    centred = matrix - average
    variance = lax.optimization_barrier(jnp.mean(centred * centred, axis=-1, keepdims=True))
    return centred * lax.rsqrt(variance + EPSILON) * gain_row

def attend(packed):
    query_rows, key_rows, value_rows, key_alive = packed
    scores = jnp.dot(query_rows, key_rows.T, preferred_element_type=jnp.float32) * query_rows.shape[-1] ** (-0.5)
    scores = jnp.where(key_alive[None, :], scores, NEGATIVE)
    row_max = lax.optimization_barrier(jnp.max(scores, axis=1))
    weights = jnp.where(key_alive[None, :], jnp.exp(scores - row_max[:, None]), 0.0)
    row_sum = lax.optimization_barrier(jnp.sum(weights, axis=1))
    numerator = jnp.dot(weights.astype(jnp.bfloat16), value_rows, preferred_element_type=jnp.float32)
    return (row_max, row_sum, numerator)

def branch(query_rows, key_rows, value_rows, offsets, valid_tile_count, seg_len, dilation):
    head_count, length, head_size = query_rows.shape
    segments = length // seg_len
    per_segment = seg_len // dilation
    chosen_mod = (offsets % dilation).astype(jnp.int32)
    picker = jnp.broadcast_to(chosen_mod[:, None, None, None, None], (head_count, segments, per_segment, 1, head_size))

    def select(matrix):
        tiled = matrix.reshape(head_count, segments, per_segment, dilation, head_size)
        return jnp.take_along_axis(tiled, picker, axis=3)[:, :, :, 0, :].reshape(head_count * segments, per_segment, head_size)
    positions = jnp.arange(segments, dtype=jnp.int32)[None, :, None] * seg_len + jnp.arange(per_segment, dtype=jnp.int32)[None, None, :] * dilation + chosen_mod[:, None, None]
    key_alive = (positions < valid_tile_count).reshape(head_count * segments, per_segment)
    row_max, row_sum, numerator = lax.map(attend, (select(query_rows), select(key_rows), select(value_rows), key_alive))
    onehot = jnp.arange(dilation, dtype=jnp.int32)[None, :] == chosen_mod[:, None]
    row_max = jnp.where(onehot[:, None, None, :], row_max.reshape(head_count, segments, per_segment, 1), NEGATIVE)
    row_sum = jnp.where(onehot[:, None, None, :], row_sum.reshape(head_count, segments, per_segment, 1), 0.0)
    numerator = jnp.where(onehot[:, None, None, :, None], numerator.reshape(head_count, segments, per_segment, 1, head_size), 0.0)
    return (row_max.reshape(head_count, length), row_sum.reshape(head_count, length), numerator.reshape(head_count, length, head_size))

def reference(tile_embed, valid_tiles, offsets, norm_gain, w_qkv, sub_gain, w_out):
    relaid = tile_embed.reshape(N_SEQ, DEVICE_TOKENS, D).transpose(1, 0, 2).reshape(SLIDE_TOKENS, D)
    normed = layer_norm(relaid.astype(jnp.float32), norm_gain).astype(jnp.bfloat16)
    projected = jnp.dot(normed, w_qkv, preferred_element_type=jnp.float32).astype(jnp.bfloat16)
    triple = projected.reshape(SLIDE_TOKENS, 3, HEADS, D // HEADS).transpose(1, 2, 0, 3)
    valid_tile_count = valid_tiles[0]
    exchange_plans = [(NEAR_SPAN * DEVICE_TOKENS, 1), (MIDDLE_SPAN * DEVICE_TOKENS, MIDDLE_DILATION), (FAR_SEGMENT_SPAN * DEVICE_TOKENS, FAR_DILATION), (SLIDE_TOKENS, FAR_DILATION)]
    branch_list = [branch(triple[0], triple[1], triple[2], offsets, valid_tile_count, seg_len, dilation) for seg_len, dilation in exchange_plans]
    highest = branch_list[0][0]
    for result in branch_list[1:]:
        highest = jnp.maximum(highest, result[0])
    denom = jnp.zeros_like(highest)
    numer_all = jnp.zeros_like(branch_list[0][2])
    for result in branch_list:
        factor = jnp.exp(result[0] - highest)
        denom = denom + factor * result[1]
        numer_all = numer_all + factor[:, :, None] * result[2]
    attended = (numer_all / jnp.maximum(denom, 1.0)[:, :, None]).astype(jnp.bfloat16)
    flattened = attended.transpose(1, 0, 2).reshape(SLIDE_TOKENS, D)
    sub_normed = layer_norm(flattened.astype(jnp.float32), sub_gain).astype(jnp.bfloat16)
    return (relaid.astype(jnp.float32) + jnp.dot(sub_normed, w_out, preferred_element_type=jnp.float32)).astype(jnp.bfloat16)
```

```python
import math

import jax
import jax.numpy as jnp
from jax import lax
from jax.experimental import pallas as pl
from jax.experimental.pallas import tpu as pltpu
from jax.sharding import Mesh, PartitionSpec as P


HEADS = 16
HEAD = 48
WIDE = 64
ROWS = 512
WIDTH = 768
NEGATIVE = -1e30
EPSILON = 1e-05
SCALE = math.log2(math.e) / math.sqrt(HEAD)
BF = jnp.bfloat16
F32 = jnp.float32


def norm_rows(x, gain):
    mean = jnp.mean(x, axis=-1, keepdims=True)
    centred = x - mean
    var = jnp.mean(centred * centred, axis=-1, keepdims=True)
    return centred * lax.rsqrt(var + EPSILON) * gain


def lanes(shape):
    return lax.broadcasted_iota(jnp.int32, shape, len(shape) - 1)


def mask_key_value(k, v, first, valid):
    lane = lanes(k.shape)
    special = lane % WIDE == HEAD
    alive = first + lax.broadcasted_iota(jnp.int32, k.shape, 0) < valid
    k = jnp.where(special, jnp.where(alive, 0.0, NEGATIVE), k)
    v = jnp.where(alive, jnp.where(special, 1.0, v), 0.0)
    return k, v


def nt(a, b):
    return lax.dot_general(a, b, (((1,), (1,)), ((), ())), preferred_element_type=F32)


def project_kernel(s_ref, x_ref, gain_ref, w_ref, own_ref, mid_ref, far_ref, normed, stage):
    p = pl.program_id(0)

    @pl.when(p == 0)
    def _():
        normed[...] = norm_rows(x_ref[...].astype(F32), gain_ref[...]).astype(BF)

    rows = normed[...]
    k = jnp.dot(rows, w_ref[0], preferred_element_type=F32).astype(BF).astype(F32)
    v = jnp.dot(rows, w_ref[1], preferred_element_type=F32).astype(BF).astype(F32)
    q = jnp.dot(rows, w_ref[2], preferred_element_type=F32).astype(BF).astype(F32)
    k, v = mask_key_value(k, v, s_ref[1] * ROWS, s_ref[0])
    q = jnp.where(lanes(q.shape) % WIDE == HEAD, 1.0, q)
    stage[0] = k
    stage[1] = v
    stage[2] = q
    own_ref[0] = k.astype(BF)
    own_ref[1] = v.astype(BF)
    own_ref[2] = q.astype(BF)
    low = lanes((ROWS // 4, 128)) < WIDE
    off = [s_ref[2 + 2 * p + a] for a in range(2)]
    for j in range(3):
        first = stage[j, pl.ds(off[0] % 4, ROWS // 4, stride=4), :]
        second = stage[j, pl.ds(off[1] % 4, ROWS // 4, stride=4), :]
        chosen = jnp.where(low, first, second).astype(BF).T
        mid_ref[0, j, :HEAD] = chosen[:HEAD]
        mid_ref[0, j, HEAD:] = chosen[WIDE : WIDE + HEAD]
    low = lanes((ROWS // 16, 128)) < WIDE
    for a in range(2):
        k, v, q = [stage[j, pl.ds(off[a] % 16, ROWS // 16, stride=16), :] for j in range(3)]
        if a == 0:
            v = pltpu.roll(v, WIDE, 1)
            q_high = pltpu.roll(q, WIDE, 1)
        else:
            k = pltpu.roll(k, WIDE, 1)
            q_high = q
            q = pltpu.roll(q, WIDE, 1)
        far_ref[a, :32] = jnp.where(low, k, v).astype(BF)
        far_ref[a, 32:] = jnp.where(low[:16], q[:16], q_high[16:]).astype(BF)


def project(scalars, rows, gain, weights):
    return pl.pallas_call(
        project_kernel,
        grid_spec=pltpu.PrefetchScalarGridSpec(
            num_scalar_prefetch=1,
            grid=(8,),
            in_specs=[
                pl.BlockSpec((ROWS, WIDTH), lambda p, s: (0, 0)),
                pl.BlockSpec((1, WIDTH), lambda p, s: (0, 0)),
                pl.BlockSpec((3, WIDTH, 128), lambda p, s: (0, 0, p)),
            ],
            out_specs=[
                pl.BlockSpec((3, ROWS, 128), lambda p, s: (0, 0, p)),
                pl.BlockSpec((1, 3, 96, 128), lambda p, s: (p, 0, 0, 0)),
                pl.BlockSpec((2, 48, 128), lambda p, s: (p, 0, 0)),
            ],
            scratch_shapes=[pltpu.VMEM((ROWS, WIDTH), BF), pltpu.VMEM((3, ROWS, 128), F32)],
        ),
        out_shape=[
            jax.ShapeDtypeStruct((3, ROWS, 1024), BF),
            jax.ShapeDtypeStruct((8, 3, 96, 128), BF),
            jax.ShapeDtypeStruct((16, 48, 128), BF),
        ],
        name="project",
    )(scalars, rows, gain, weights)


def attend(s, values_t):
    m = jnp.max(s, axis=0, keepdims=True)
    p = jnp.exp2(s * SCALE - m * SCALE).astype(BF)
    return jnp.dot(values_t, p, preferred_element_type=F32), m


def near_kernel(s_ref, x_ref, gain_ref, w_ref, own_ref, out_ref, normed):
    p = pl.program_id(0)

    @pl.when(p == 0)
    def _():
        normed[...] = norm_rows(x_ref[...].astype(F32), gain_ref[...]).astype(BF)

    rows = normed[...]
    k = jnp.dot(rows, w_ref[0], preferred_element_type=F32).astype(BF).astype(F32)
    v = jnp.dot(rows, w_ref[1], preferred_element_type=F32).astype(BF).astype(F32)
    partner = s_ref[1] + 1 - 2 * (s_ref[1] % 2)
    k, v = mask_key_value(k, v, partner * ROWS, s_ref[0])
    keys = jnp.concatenate([own_ref[0], k.astype(BF)], axis=0)
    values_t = jnp.concatenate([own_ref[1], v.astype(BF)], axis=0).T
    queries = own_ref[2]
    for a in range(2):
        for c in range(0, ROWS, 256):
            part = queries[c : c + 256]
            part = jnp.where(lanes(part.shape) // WIDE == a, part, jnp.zeros_like(part))
            numer, m = attend(nt(keys, part), values_t[a * WIDE : (a + 1) * WIDE])
            row = lax.broadcasted_iota(jnp.int32, numer.shape, 0)
            out_ref[a, :, c : c + 256] = jnp.where(row == HEAD + 1, m, numer)


def near(scalars, rows, gain, weights, own, first, count):
    return pl.pallas_call(
        near_kernel,
        grid_spec=pltpu.PrefetchScalarGridSpec(
            num_scalar_prefetch=1,
            grid=(count,),
            in_specs=[
                pl.BlockSpec((ROWS, WIDTH), lambda p, s: (0, 0)),
                pl.BlockSpec((1, WIDTH), lambda p, s: (0, 0)),
                pl.BlockSpec((2, WIDTH, 128), lambda p, s: (0, 0, p + first)),
                pl.BlockSpec((3, ROWS, 128), lambda p, s: (0, 0, p + first)),
            ],
            out_specs=pl.BlockSpec((2, WIDE, ROWS), lambda p, s: (p, 0, 0)),
            scratch_shapes=[pltpu.VMEM((ROWS, WIDTH), BF)],
        ),
        out_shape=jax.ShapeDtypeStruct((2 * count, WIDE, ROWS), F32),
        cost_estimate=pl.CostEstimate(
            flops=5_000_000_000 * count,
            bytes_accessed=1_000_000 * count,
            transcendentals=1_050_000 * count,
        ),
        name="near",
    )(scalars, rows, gain, weights, own)


def to_lse(numer, m):
    total = numer[HEAD : HEAD + 1]
    lse = jnp.where(total > 0.0, m * SCALE + jnp.log2(jnp.maximum(total, 1.0)), NEGATIVE)
    return numer / jnp.maximum(total, 1.0), lse


def packed_result(numer, m):
    mean, lse = to_lse(numer, m)
    high = lse.astype(BF).astype(F32)
    rest = lse - high
    second = rest.astype(BF).astype(F32)
    third = rest - second
    row = lax.broadcasted_iota(jnp.int32, mean.shape, 0)
    out = jnp.where(row < HEAD, mean, 0.0)
    out = jnp.where(row == HEAD, high, out)
    out = jnp.where(row == HEAD + 1, second, out)
    return jnp.where(row == HEAD + 2, third, out)


def middle_kernel(s_ref, in_ref, out_ref, keys_t, values_t, queries_t):
    column = s_ref[1] // 8
    pair = s_ref[1] % 8
    row = lax.broadcasted_iota(jnp.int32, (WIDE - HEAD, 1024), 0)
    for a in range(2):
        base = a * WIDE
        for i in range(8):
            part = slice(i * 128, (i + 1) * 128)
            for j, ref in enumerate((keys_t, values_t, queries_t)):
                ref[base : base + HEAD, part] = in_ref[i, j, a * HEAD : (a + 1) * HEAD]
        place = column * 4096 + s_ref[2 + 2 * pair + a] % 4 + 4 * lanes(row.shape)
        alive = place < s_ref[0]
        spare = slice(base + HEAD, base + WIDE)
        first = row == 0
        keys_t[spare] = jnp.where(first & (~alive), NEGATIVE, 0.0).astype(BF)
        values_t[spare] = jnp.where(first & alive, 1.0, 0.0).astype(BF)
        queries_t[spare] = jnp.where(first, 1.0, 0.0).astype(BF)
        alive = column * 4096 + s_ref[2 + 2 * pair + a] % 4 + 4 * lanes((HEAD, 1024)) < s_ref[0]
        values = values_t[base : base + HEAD]
        values_t[base : base + HEAD] = jnp.where(alive, values, jnp.zeros_like(values))
    keys = keys_t[...].T
    for c in range(0, 1024, 256):
        queries = queries_t[:, c : c + 256]
        head = lax.broadcasted_iota(jnp.int32, queries.shape, 0) // WIDE
        for a in range(2):
            part = jnp.where(head == a, queries, jnp.zeros_like(queries))
            s = jnp.dot(keys, part, preferred_element_type=F32)
            numer, m = attend(s, values_t[a * WIDE : (a + 1) * WIDE])
            out = packed_result(numer, m).astype(BF)
            for i in range(2):
                out_ref[c // 128 + i, a * WIDE : (a + 1) * WIDE] = out[:, i * 128 : (i + 1) * 128]


def middle(scalars, received):
    return pl.pallas_call(
        middle_kernel,
        grid_spec=pltpu.PrefetchScalarGridSpec(
            num_scalar_prefetch=1,
            grid=(1,),
            in_specs=[pl.BlockSpec((8, 3, 96, 128), lambda i, s: (0, 0, 0, 0))],
            out_specs=pl.BlockSpec((8, 128, 128), lambda i, s: (0, 0, 0)),
            scratch_shapes=[pltpu.VMEM((128, 1024), BF)] * 3,
        ),
        out_shape=jax.ShapeDtypeStruct((8, 128, 128), BF),
        cost_estimate=pl.CostEstimate(
            flops=10_000_000_000, bytes_accessed=1_000_000, transcendentals=2_100_000
        ),
        name="middle",
    )(scalars, received)


def far_kernel(*refs):
    key_refs = refs[:8]
    in_ref, out_ref, scores, values_t = refs[8:]
    for c in range(8):
        values_t[:, 512 * c : 512 * c + 512] = key_refs[c][...].reshape(512, 128).T[WIDE:]
    packed = in_ref[:, 32:48].reshape(256, 128)
    low = lanes(packed.shape) < WIDE
    for half in range(2):
        queries = packed.astype(F32)
        if half:
            queries = pltpu.roll(queries, WIDE, 1)
        queries = jnp.where(low, queries, 0.0).astype(BF)
        m = jnp.full((1, 256), NEGATIVE, F32)
        for c in range(8):
            s = nt(key_refs[c][...].reshape(512, 128), queries)
            scores[c] = s
            m = jnp.maximum(m, jnp.max(s, axis=0, keepdims=True))
        numer = jnp.zeros((WIDE, 256), F32)
        for c in range(8):
            shift = m * SCALE - (1.0 if c < 2 else 0.0)
            p = jnp.exp2(scores[c] * SCALE - shift).astype(BF)
            numer += jnp.dot(
                values_t[:, 512 * c : 512 * c + 512], p, preferred_element_type=F32
            )
        out = packed_result(numer, m)
        out = jnp.concatenate([out, jnp.zeros_like(out)], axis=0).T
        out_ref[:, 16 * half : 16 * half + 16] = out.astype(BF).reshape(16, 16, 128)


def far(keys, received):
    return pl.pallas_call(
        far_kernel,
        out_shape=jax.ShapeDtypeStruct((16, 32, 128), BF),
        scratch_shapes=[pltpu.VMEM((8, 512, 256), F32), pltpu.VMEM((WIDE, 4096), BF)],
        cost_estimate=pl.CostEstimate(
            flops=10_000_000_000, bytes_accessed=1_000_000, transcendentals=2_100_000
        ),
        name="far",
    )(*keys, received)


def finish_kernel(s_ref, near0_ref, near1_ref, near2_ref, mid_ref, far_ref, x_ref, gain_ref, w_ref, out_ref, mixed):
    lane = lanes((1, ROWS))
    column4 = lanes((128, ROWS)) - 4 * lax.broadcasted_iota(jnp.int32, (128, ROWS), 0)
    column16 = lanes((32, ROWS)) - 16 * lax.broadcasted_iota(jnp.int32, (32, ROWS), 0)
    for h in range(HEADS):
        off = s_ref[2 + h]
        off4 = off % 4
        off16 = off % 16
        near_ref = (near0_ref, near1_ref, near2_ref)[h // 6]
        mean_n, lse_n = to_lse(near_ref[h % 6], near_ref[h % 6, HEAD + 1 : HEAD + 2])
        a = h % 2
        spread4 = jnp.where(column4 == off4, 1.0, 0.0).astype(BF)
        mid = jnp.dot(
            mid_ref[h // 2, a * WIDE : (a + 1) * WIDE], spread4, preferred_element_type=F32
        )
        spread16 = jnp.where(column16 == off16, 1.0, 0.0).astype(BF)
        distant = lax.dot_general(
            far_ref[h], spread16, (((0,), (0,)), ((), ())), preferred_element_type=F32
        )

        def lse_of(spread):
            lse = spread[HEAD : HEAD + 1] + spread[HEAD + 1 : HEAD + 2]
            return lse + spread[HEAD + 2 : HEAD + 3]

        lse_m = jnp.where(lane % 4 == off4, lse_of(mid), NEGATIVE)
        lse_f = jnp.where(lane % 16 == off16, lse_of(distant), NEGATIVE)
        top = jnp.maximum(jnp.maximum(lse_n, lse_m), lse_f)
        weight_n = jnp.exp2(lse_n - top)
        weight_m = jnp.exp2(lse_m - top)
        weight_f = jnp.exp2(lse_f - top)
        inverse = 1.0 / jnp.maximum(weight_n + weight_m + weight_f, 1.0)
        mixed[HEAD * h : HEAD * (h + 1)] = (
            mean_n[:HEAD] * (weight_n * inverse)
            + mid[:HEAD] * (weight_m * inverse)
            + distant[:HEAD] * (weight_f * inverse)
        ).astype(BF)
    attended = mixed[...].T.astype(F32)
    sub = norm_rows(attended, gain_ref[...]).astype(BF)
    out = x_ref[...].astype(F32) + jnp.dot(sub, w_ref[...], preferred_element_type=F32)
    out_ref[...] = out.astype(BF)


def finish(scalars, near_results, mid_result, far_result, rows, gain, w_out):
    def whole(*shape):
        return pl.BlockSpec(shape, lambda i, s: (0,) * len(shape))

    return pl.pallas_call(
        finish_kernel,
        grid_spec=pltpu.PrefetchScalarGridSpec(
            num_scalar_prefetch=1,
            grid=(1,),
            in_specs=[
                whole(6, WIDE, ROWS),
                whole(6, WIDE, ROWS),
                whole(4, WIDE, ROWS),
                whole(8, 128, 128),
                whole(16, 32, 128),
                whole(ROWS, WIDTH),
                whole(1, WIDTH),
                whole(WIDTH, WIDTH),
            ],
            out_specs=whole(ROWS, WIDTH),
            scratch_shapes=[pltpu.VMEM((WIDTH, ROWS), BF)],
        ),
        out_shape=jax.ShapeDtypeStruct((ROWS, WIDTH), BF),
        name="finish",
    )(scalars, *near_results, mid_result, far_result, rows, gain, w_out)


def exchange(value, axis):
    return lax.all_to_all(value, axis, split_axis=0, concat_axis=0, tiled=True)


def body(tile_embed, valid_tiles, offsets, norm_gain, w_qkv, sub_gain, w_out):
    position = lax.axis_index(("y", "xh", "xl", "z"))
    scalars = jnp.concatenate([valid_tiles, position.astype(jnp.int32)[None], offsets])
    arrived = exchange(tile_embed.reshape(128, 4, WIDTH), ("y", "xh", "xl", "z"))
    rows = arrived.transpose(1, 0, 2).reshape(ROWS, WIDTH)
    partner = lax.ppermute(rows, "z", [(i, i ^ 1) for i in range(8)])
    wide = w_qkv.reshape(WIDTH, 3, HEADS, HEAD)
    wide = jnp.pad(wide, ((0, 0), (0, 0), (0, 0), (0, WIDE - HEAD))).reshape(WIDTH, 3, 1024)
    weights = jnp.stack([wide[:, 1], wide[:, 2], wide[:, 0]])
    gain = norm_gain[None]
    own, mid_send, far_send = project(scalars, rows, gain, weights)
    received = exchange(far_send, ("xl", "z"))
    mine = received[:, :32]
    keys = [mine]
    for y in range(4):
        for xh in range(2):
            if y or xh:
                moves = [
                    (2 * i + j, 2 * ((i + y) % 4) + (j ^ xh)) for i in range(4) for j in range(2)
                ]
                keys.append(lax.ppermute(mine, ("y", "xh"), moves))
    mid = exchange(mid_send, "z")
    near_results = []
    for first, count in ((0, 3), (3, 3), (6, 2)):
        near_results.append(near(scalars, partner, gain, weights, own, first, count))
    mid_result = middle(scalars, mid)
    far_result = far(keys, received)
    mid_result = exchange(mid_result, "z")
    far_result = exchange(far_result, ("xl", "z"))
    return finish(
        scalars, near_results, mid_result, far_result, rows, sub_gain[None], w_out
    )


def solution(mesh):
    inner = Mesh(mesh.devices.reshape(4, 2, 2, 8, 2), ("y", "xh", "xl", "z", "slide"))
    split = P(("slide", "y", "xh", "xl", "z"), None)
    return jax.shard_map(
        body,
        mesh=inner,
        in_specs=(split, P("slide"), P(), P(), P(), P(), P()),
        out_specs=split,
        check_vma=False,
    )
```

```python
import math

import jax
import jax.numpy as jnp
from jax import lax
from jax.experimental import pallas as pl
from jax.experimental.pallas import tpu as pltpu
from jax.sharding import Mesh, PartitionSpec as P


HEADS = 16
HEAD = 48
WIDE = 64
ROWS = 512
WIDTH = 768
NEGATIVE = -1e30
EPSILON = 1e-05
SCALE = math.log2(math.e) / math.sqrt(HEAD)
BF = jnp.bfloat16
F32 = jnp.float32


def norm_rows(x, gain):
    mean = jnp.mean(x, axis=-1, keepdims=True)
    centred = x - mean
    var = jnp.mean(centred * centred, axis=-1, keepdims=True)
    return centred * lax.rsqrt(var + EPSILON) * gain


def lanes(shape):
    return lax.broadcasted_iota(jnp.int32, shape, len(shape) - 1)


def mask_key_value(k, v, first, valid):
    lane = lanes(k.shape)
    special = lane % WIDE == HEAD
    alive = first + lax.broadcasted_iota(jnp.int32, k.shape, 0) < valid
    k = jnp.where(special, jnp.where(alive, 0.0, NEGATIVE), k)
    v = jnp.where(alive, jnp.where(special, 1.0, v), 0.0)
    return k, v


def nt(a, b):
    return lax.dot_general(a, b, (((1,), (1,)), ((), ())), preferred_element_type=F32)


def project_kernel(s_ref, x_ref, gain_ref, w_ref, own_ref, send_ref, normed, stage):
    p = pl.program_id(0)

    @pl.when(p == 0)
    def _():
        normed[...] = norm_rows(x_ref[...].astype(F32), gain_ref[...]).astype(BF)

    rows = normed[...]
    k = jnp.dot(rows, w_ref[0], preferred_element_type=F32).astype(BF).astype(F32)
    v = jnp.dot(rows, w_ref[1], preferred_element_type=F32).astype(BF).astype(F32)
    q = jnp.dot(rows, w_ref[2], preferred_element_type=F32).astype(BF).astype(F32)
    k, v = mask_key_value(k, v, s_ref[1] * ROWS, s_ref[0])
    q = jnp.where(lanes(q.shape) % WIDE == HEAD, 1.0, q)
    stage[0] = k
    stage[1] = v
    stage[2] = q
    own_ref[0] = k.astype(BF)
    own_ref[1] = v.astype(BF)
    own_ref[2] = q.astype(BF)
    low = lanes((ROWS // 4, 128)) < WIDE
    off = [s_ref[2 + 2 * p + a] for a in range(2)]
    for j in range(3):
        first = stage[j, pl.ds(off[0] % 4, ROWS // 4, stride=4), :]
        second = stage[j, pl.ds(off[1] % 4, ROWS // 4, stride=4), :]
        chosen = jnp.where(low, first, second).astype(BF).T
        for a in range(2):
            send_ref[a, HEAD * (j + 1) : HEAD * (j + 2)] = chosen[a * WIDE : a * WIDE + HEAD]
    low = lanes((ROWS // 16, 128)) < WIDE
    for a in range(2):
        k, v, q = [stage[j, pl.ds(off[a] % 16, ROWS // 16, stride=16), :] for j in range(3)]
        if a == 0:
            v = pltpu.roll(v, WIDE, 1)
            q_high = pltpu.roll(q, WIDE, 1)
        else:
            k = pltpu.roll(k, WIDE, 1)
            q_high = q
            q = pltpu.roll(q, WIDE, 1)
        send_ref[a, :32] = jnp.where(low, k, v).astype(BF)
        send_ref[a, 32:48] = jnp.where(low[:16], q[:16], q_high[16:]).astype(BF)


def project(scalars, rows, gain, weights):
    return pl.pallas_call(
        project_kernel,
        grid_spec=pltpu.PrefetchScalarGridSpec(
            num_scalar_prefetch=1,
            grid=(8,),
            in_specs=[
                pl.BlockSpec((ROWS, WIDTH), lambda p, s: (0, 0)),
                pl.BlockSpec((1, WIDTH), lambda p, s: (0, 0)),
                pl.BlockSpec((3, WIDTH, 128), lambda p, s: (0, 0, p)),
            ],
            out_specs=[
                pl.BlockSpec((3, ROWS, 128), lambda p, s: (0, 0, p)),
                pl.BlockSpec((2, 192, 128), lambda p, s: (p, 0, 0)),
            ],
            scratch_shapes=[pltpu.VMEM((ROWS, WIDTH), BF), pltpu.VMEM((3, ROWS, 128), F32)],
        ),
        out_shape=[
            jax.ShapeDtypeStruct((3, ROWS, 1024), BF),
            jax.ShapeDtypeStruct((16, 192, 128), BF),
        ],
        name="project",
    )(scalars, rows, gain, weights)


def attend(score, values_t, scores, weights, bonus=()):
    blocks = scores.shape[0] // 256
    m = None
    for c in range(blocks):
        s = score(c)
        scores[256 * c : 256 * c + 256] = s
        part = jnp.max(s.reshape(32, 8, s.shape[1]), axis=0)
        m = part if m is None else jnp.maximum(m, part)
    m = jnp.max(m, axis=0, keepdims=True)
    for c in range(blocks):
        shift = m * SCALE - (1.0 if c in bonus else 0.0)
        block = slice(256 * c, 256 * c + 256)
        weights[block] = jnp.exp2(scores[block] * SCALE - shift).astype(BF)
    return jnp.dot(values_t, weights[...], preferred_element_type=F32), m


def near_kernel(s_ref, x_ref, gain_ref, w_ref, own_ref, out_ref, normed, keys, scores, weights):
    p = pl.program_id(0)

    @pl.when(p == 0)
    def _():
        normed[...] = norm_rows(x_ref[...].astype(F32), gain_ref[...]).astype(BF)

    rows = normed[...]
    k = jnp.dot(rows, w_ref[0], preferred_element_type=F32).astype(BF).astype(F32)
    v = jnp.dot(rows, w_ref[1], preferred_element_type=F32).astype(BF).astype(F32)
    partner = s_ref[1] + 1 - 2 * (s_ref[1] % 2)
    k, v = mask_key_value(k, v, partner * ROWS, s_ref[0])
    keys[:ROWS] = own_ref[0]
    keys[ROWS:] = k.astype(BF)
    values_t = jnp.concatenate([own_ref[1], v.astype(BF)], axis=0).T
    queries = own_ref[2]
    for a in range(2):
        for c in range(0, ROWS, 256):
            part = queries[c : c + 256]
            part = jnp.where(lanes(part.shape) // WIDE == a, part, jnp.zeros_like(part))
            slot = (2 * a + c // 256) % 2
            numer, m = attend(
                lambda i: nt(keys[256 * i : 256 * i + 256], part),
                values_t[a * WIDE : (a + 1) * WIDE],
                scores.at[slot],
                weights.at[slot],
            )
            row = lax.broadcasted_iota(jnp.int32, numer.shape, 0)
            out_ref[a, :, c : c + 256] = jnp.where(row == HEAD + 1, m, numer)


def near(scalars, rows, gain, weights, own, first, count):
    return pl.pallas_call(
        near_kernel,
        grid_spec=pltpu.PrefetchScalarGridSpec(
            num_scalar_prefetch=1,
            grid=(count,),
            in_specs=[
                pl.BlockSpec((ROWS, WIDTH), lambda p, s: (0, 0)),
                pl.BlockSpec((1, WIDTH), lambda p, s: (0, 0)),
                pl.BlockSpec((2, WIDTH, 128), lambda p, s: (0, 0, p + first)),
                pl.BlockSpec((3, ROWS, 128), lambda p, s: (0, 0, p + first)),
            ],
            out_specs=pl.BlockSpec((2, WIDE, ROWS), lambda p, s: (p, 0, 0)),
            scratch_shapes=[
                pltpu.VMEM((ROWS, WIDTH), BF),
                pltpu.VMEM((2 * ROWS, 128), BF),
                pltpu.VMEM((2, 2 * ROWS, 256), F32),
                pltpu.VMEM((2, 2 * ROWS, 256), BF),
            ],
        ),
        out_shape=jax.ShapeDtypeStruct((2 * count, WIDE, ROWS), F32),
        cost_estimate=pl.CostEstimate(
            flops=5_000_000_000 * count,
            bytes_accessed=1_000_000 * count,
            transcendentals=1_050_000 * count,
        ),
        name="near",
    )(scalars, rows, gain, weights, own)


def to_lse(numer, m):
    total = numer[HEAD : HEAD + 1]
    lse = jnp.where(total > 0.0, m * SCALE + jnp.log2(jnp.maximum(total, 1.0)), NEGATIVE)
    return numer / jnp.maximum(total, 1.0), lse


def packed_result(numer, m):
    mean, lse = to_lse(numer, m)
    high = lse.astype(BF).astype(F32)
    rest = lse - high
    second = rest.astype(BF).astype(F32)
    third = rest - second
    row = lax.broadcasted_iota(jnp.int32, mean.shape, 0)
    out = jnp.where(row < HEAD, mean, 0.0)
    out = jnp.where(row == HEAD, high, out)
    out = jnp.where(row == HEAD + 1, second, out)
    return jnp.where(row == HEAD + 2, third, out)


def middle_kernel(s_ref, in_ref, out_ref, keys_t, values_t, queries_t, keys, scores, weights):
    off4 = s_ref[2 + s_ref[1] % HEADS] % 4
    row = lax.broadcasted_iota(jnp.int32, (WIDE - HEAD, 1024), 0)
    first = row == 0
    for g in range(2):
        base = g * WIDE
        for i in range(8):
            part = slice(i * 128, (i + 1) * 128)
            for j, ref in enumerate((keys_t, values_t, queries_t)):
                ref[base : base + HEAD, part] = in_ref[8 * g + i, HEAD * (j + 1) : HEAD * (j + 2)]
        start = (s_ref[1] // HEADS * 2 + g) * 4096 + off4
        alive = start + 4 * lanes(row.shape) < s_ref[0]
        spare = slice(base + HEAD, base + WIDE)
        keys_t[spare] = jnp.where(first & (~alive), NEGATIVE, 0.0).astype(BF)
        values_t[spare] = jnp.where(first & alive, 1.0, 0.0).astype(BF)
        queries_t[spare] = jnp.where(first, 1.0, 0.0).astype(BF)
        alive = start + 4 * lanes((HEAD, 1024)) < s_ref[0]
        values = values_t[base : base + HEAD]
        values_t[base : base + HEAD] = jnp.where(alive, values, jnp.zeros_like(values))
    keys[...] = keys_t[...].T
    for c in range(0, 1024, 256):
        queries = queries_t[:, c : c + 256]
        owner = lax.broadcasted_iota(jnp.int32, queries.shape, 0) // WIDE
        for g in range(2):
            part = jnp.where(owner == g, queries, jnp.zeros_like(queries))
            numer, m = attend(
                lambda i: jnp.dot(
                    keys[256 * i : 256 * i + 256], part, preferred_element_type=F32
                ),
                values_t[g * WIDE : (g + 1) * WIDE],
                scores.at[g],
                weights.at[g],
            )
            out = packed_result(numer, m).astype(BF)
            for i in range(2):
                out_ref[8 * g + c // 128 + i] = out[:, i * 128 : (i + 1) * 128]


def middle(scalars, received):
    return pl.pallas_call(
        middle_kernel,
        grid_spec=pltpu.PrefetchScalarGridSpec(
            num_scalar_prefetch=1,
            grid=(1,),
            in_specs=[pl.BlockSpec((16, 192, 128), lambda i, s: (0, 0, 0))],
            out_specs=pl.BlockSpec((16, WIDE, 128), lambda i, s: (0, 0, 0)),
            scratch_shapes=[pltpu.VMEM((128, 1024), BF)] * 3
            + [
                pltpu.VMEM((1024, 128), BF),
                pltpu.VMEM((2, 1024, 256), F32),
                pltpu.VMEM((2, 1024, 256), BF),
            ],
        ),
        out_shape=jax.ShapeDtypeStruct((16, WIDE, 128), BF),
        cost_estimate=pl.CostEstimate(
            flops=10_000_000_000, bytes_accessed=1_000_000, transcendentals=2_100_000
        ),
        name="middle",
    )(scalars, received)


def far_kernel(own_ref, *refs):
    key_refs = (own_ref,) + refs[:3]
    in_ref, mid_ref, out_ref, scores, weights, values_t = refs[3:]
    for c in range(8):
        block = key_refs[c // 2][16 * (c % 2) : 16 * (c % 2) + 16].reshape(512, 128)
        values_t[:, 512 * c : 512 * c + 512] = block.T[WIDE:]
    packed = in_ref[:, 32:48].reshape(256, 128).astype(F32)
    low = lanes(packed.shape) < WIDE
    for half in range(2):
        queries = pltpu.roll(packed, WIDE, 1) if half else packed
        queries = jnp.where(low, queries, 0.0).astype(BF)

        def score(c):
            block = key_refs[c // 4][8 * (c % 4) : 8 * (c % 4) + 8]
            return nt(block.reshape(256, 128), queries)

        numer, m = attend(score, values_t[...], scores.at[half], weights.at[half], range(4))
        out = packed_result(numer, m)
        out = jnp.concatenate([out, jnp.zeros_like(out)], axis=0).T
        out_ref[:, 16 * half : 16 * half + 16] = out.astype(BF).reshape(16, 16, 128)
    out_ref[:, 32:] = mid_ref[...]


def far(keys, received, mid_result):
    return pl.pallas_call(
        far_kernel,
        out_shape=jax.ShapeDtypeStruct((16, 96, 128), BF),
        scratch_shapes=[
            pltpu.VMEM((2, 4096, 256), F32),
            pltpu.VMEM((2, 4096, 256), BF),
            pltpu.VMEM((WIDE, 4096), BF),
        ],
        cost_estimate=pl.CostEstimate(
            flops=10_000_000_000, bytes_accessed=1_000_000, transcendentals=2_100_000
        ),
        name="far",
    )(*keys, received, mid_result)


def finish_kernel(s_ref, near0_ref, near1_ref, near2_ref, in_ref, x_ref, gain_ref, w_ref, out_ref, mixed):
    lane = lanes((1, ROWS))
    column4 = lanes((128, ROWS)) - 4 * lax.broadcasted_iota(jnp.int32, (128, ROWS), 0)
    column16 = lanes((32, ROWS)) - 16 * lax.broadcasted_iota(jnp.int32, (32, ROWS), 0)
    for h in range(HEADS):
        off = s_ref[2 + h]
        off4 = off % 4
        off16 = off % 16
        near_ref = (near0_ref, near1_ref, near2_ref)[h // 6]
        mean_n, lse_n = to_lse(near_ref[h % 6], near_ref[h % 6, HEAD + 1 : HEAD + 2])
        spread4 = jnp.where(column4 == off4, 1.0, 0.0).astype(BF)
        mid = jnp.dot(
            in_ref[h, 32:], spread4, preferred_element_type=F32
        )
        spread16 = jnp.where(column16 == off16, 1.0, 0.0).astype(BF)
        distant = lax.dot_general(
            in_ref[h, :32], spread16, (((0,), (0,)), ((), ())), preferred_element_type=F32
        )

        def lse_of(spread):
            lse = spread[HEAD : HEAD + 1] + spread[HEAD + 1 : HEAD + 2]
            return lse + spread[HEAD + 2 : HEAD + 3]

        lse_m = jnp.where(lane % 4 == off4, lse_of(mid), NEGATIVE)
        lse_f = jnp.where(lane % 16 == off16, lse_of(distant), NEGATIVE)
        top = jnp.maximum(jnp.maximum(lse_n, lse_m), lse_f)
        weight_n = jnp.exp2(lse_n - top)
        weight_m = jnp.exp2(lse_m - top)
        weight_f = jnp.exp2(lse_f - top)
        inverse = 1.0 / jnp.maximum(weight_n + weight_m + weight_f, 1.0)
        mixed[HEAD * h : HEAD * (h + 1)] = (
            mean_n[:HEAD] * (weight_n * inverse)
            + mid[:HEAD] * (weight_m * inverse)
            + distant[:HEAD] * (weight_f * inverse)
        ).astype(BF)
    attended = mixed[...].T.astype(F32)
    sub = norm_rows(attended, gain_ref[...]).astype(BF)
    out = x_ref[...].astype(F32) + jnp.dot(sub, w_ref[...], preferred_element_type=F32)
    out_ref[...] = out.astype(BF)


def finish(scalars, near_results, dilated, rows, gain, w_out):
    def whole(*shape):
        return pl.BlockSpec(shape, lambda i, s: (0,) * len(shape))

    return pl.pallas_call(
        finish_kernel,
        grid_spec=pltpu.PrefetchScalarGridSpec(
            num_scalar_prefetch=1,
            grid=(1,),
            in_specs=[
                whole(6, WIDE, ROWS),
                whole(6, WIDE, ROWS),
                whole(4, WIDE, ROWS),
                whole(16, 96, 128),
                whole(ROWS, WIDTH),
                whole(1, WIDTH),
                whole(WIDTH, WIDTH),
            ],
            out_specs=whole(ROWS, WIDTH),
            scratch_shapes=[pltpu.VMEM((WIDTH, ROWS), BF)],
        ),
        out_shape=jax.ShapeDtypeStruct((ROWS, WIDTH), BF),
        name="finish",
    )(scalars, *near_results, dilated, rows, gain, w_out)


def exchange(value, axis):
    return lax.all_to_all(value, axis, split_axis=0, concat_axis=0, tiled=True)


def body(tile_embed, valid_tiles, offsets, norm_gain, w_qkv, sub_gain, w_out):
    position = lax.axis_index(("y", "xh", "xl", "z"))
    scalars = jnp.concatenate([valid_tiles, position.astype(jnp.int32)[None], offsets])
    arrived = exchange(tile_embed.reshape(128, 4, WIDTH), ("y", "xh", "xl", "z"))
    rows = arrived.transpose(1, 0, 2).reshape(ROWS, WIDTH)
    partner = lax.ppermute(rows, "z", [(i, i ^ 1) for i in range(8)])
    wide = w_qkv.reshape(WIDTH, 3, HEADS, HEAD)
    wide = jnp.pad(wide, ((0, 0), (0, 0), (0, 0), (0, WIDE - HEAD))).reshape(WIDTH, 3, 1024)
    weights = jnp.stack([wide[:, 1], wide[:, 2], wide[:, 0]])
    gain = norm_gain[None]
    own, send = project(scalars, rows, gain, weights)
    received = exchange(send, ("xl", "z"))
    mine = received[:, :32]
    other = lax.ppermute(mine, "xh", [(0, 1), (1, 0)])
    keys = [jnp.concatenate([mine, other])]
    for y in range(1, 4):
        keys.append(lax.ppermute(keys[0], "y", [(i, (i + y) % 4) for i in range(4)]))
    near_results = []
    for first, count in ((0, 3), (3, 3), (6, 2)):
        near_results.append(near(scalars, partner, gain, weights, own, first, count))
    mid_result = middle(scalars, received)
    far_result = far(keys, received, mid_result)
    dilated = exchange(far_result, ("xl", "z"))
    return finish(scalars, near_results, dilated, rows, sub_gain[None], w_out)


def solution(mesh):
    inner = Mesh(mesh.devices.reshape(4, 2, 2, 8, 2), ("y", "xh", "xl", "z", "slide"))
    split = P(("slide", "y", "xh", "xl", "z"), None)
    return jax.shard_map(
        body,
        mesh=inner,
        in_specs=(split, P("slide"), P(), P(), P(), P(), P()),
        out_specs=split,
        check_vma=False,
    )
```

```python
import math

import jax
import jax.numpy as jnp
from jax import lax
from jax.experimental import pallas as pl
from jax.experimental.pallas import tpu as pltpu
from jax.sharding import Mesh, PartitionSpec as P


HEADS = 16
HEAD = 48
WIDE = 64
ROWS = 512
WIDTH = 768
NEGATIVE = -1e30
EPSILON = 1e-05
SCALE = math.log2(math.e) / math.sqrt(HEAD)
BF = jnp.bfloat16
F32 = jnp.float32


def norm_rows(x, gain):
    mean = jnp.mean(x, axis=-1, keepdims=True)
    centred = x - mean
    var = jnp.mean(centred * centred, axis=-1, keepdims=True)
    return centred * lax.rsqrt(var + EPSILON) * gain


def lanes(shape):
    return lax.broadcasted_iota(jnp.int32, shape, len(shape) - 1)


def mask_key_value(k, v, first, valid):
    lane = lanes(k.shape)
    special = lane % WIDE == HEAD
    alive = first + lax.broadcasted_iota(jnp.int32, k.shape, 0) < valid
    k = jnp.where(special, jnp.where(alive, 0.0, NEGATIVE), k)
    v = jnp.where(alive, jnp.where(special, 1.0, v), 0.0)
    return k, v


def nt(a, b):
    return lax.dot_general(a, b, (((1,), (1,)), ((), ())), preferred_element_type=F32)


def widen_kernel(w_ref, out_ref):
    for j, start in enumerate((WIDTH, 2 * WIDTH, 0)):
        for p in range(8):
            first = start + 2 * HEAD * p
            window = first // 128 * 128
            row = lax.broadcasted_iota(jnp.int32, (256, 128), 0) + (window - first)
            lane = lanes((256, 128))
            column = lane % WIDE + lane // WIDE * HEAD
            chosen = (row == column) & (lane % WIDE < HEAD)
            pick = jnp.where(chosen, 1.0, 0.0).astype(BF)
            wide = min(256, 3 * WIDTH - window)
            part = jnp.dot(
                w_ref[:, window : window + wide], pick[:wide], preferred_element_type=F32
            )
            out_ref[p, j] = part.astype(BF)


def widen(w_qkv):
    return pl.pallas_call(
        widen_kernel,
        out_shape=jax.ShapeDtypeStruct((8, 3, WIDTH, 128), BF),
        cost_estimate=pl.CostEstimate(
            flops=10_000_000_000, bytes_accessed=8_000_000, transcendentals=0
        ),
        name="widen",
    )(w_qkv)


def project_kernel(s_ref, x_ref, gain_ref, w_ref, own_ref, send_ref, normed, stage):
    p = pl.program_id(0)

    @pl.when(p == 0)
    def _():
        normed[...] = norm_rows(x_ref[...].astype(F32), gain_ref[...]).astype(BF)

    rows = normed[...]
    k = jnp.dot(rows, w_ref[0, 0], preferred_element_type=F32).astype(BF).astype(F32)
    v = jnp.dot(rows, w_ref[0, 1], preferred_element_type=F32).astype(BF).astype(F32)
    q = (jnp.dot(rows, w_ref[0, 2], preferred_element_type=F32) * SCALE).astype(BF).astype(F32)
    k, v = mask_key_value(k, v, s_ref[1] * ROWS, s_ref[0])
    q = jnp.where(lanes(q.shape) % WIDE == HEAD, 1.0, q)
    stage[0] = k
    stage[1] = v
    stage[2] = q
    own_ref[0, 0] = k.astype(BF)
    own_ref[0, 1] = v.astype(BF)
    own_ref[0, 2] = q.astype(BF)
    low = lanes((ROWS // 4, 128)) < WIDE
    off = [s_ref[2 + 2 * p + a] for a in range(2)]
    for j in range(3):
        first = stage[j, pl.ds(off[0] % 4, ROWS // 4, stride=4), :]
        second = stage[j, pl.ds(off[1] % 4, ROWS // 4, stride=4), :]
        chosen = jnp.where(low, first, second).astype(BF).T
        for a in range(2):
            send_ref[a, HEAD * (j + 1) : HEAD * (j + 2)] = chosen[a * WIDE : a * WIDE + HEAD]
    low = lanes((ROWS // 16, 128)) < WIDE
    for a in range(2):
        k, v, q = [stage[j, pl.ds(off[a] % 16, ROWS // 16, stride=16), :] for j in range(3)]
        if a == 0:
            v = pltpu.roll(v, WIDE, 1)
            q_high = pltpu.roll(q, WIDE, 1)
        else:
            k = pltpu.roll(k, WIDE, 1)
            q_high = q
            q = pltpu.roll(q, WIDE, 1)
        send_ref[a, :32] = jnp.where(low, k, v).astype(BF)
        send_ref[a, 32:48] = jnp.where(low[:16], q[:16], q_high[16:]).astype(BF)


def project(scalars, rows, gain, weights):
    return pl.pallas_call(
        project_kernel,
        grid_spec=pltpu.PrefetchScalarGridSpec(
            num_scalar_prefetch=1,
            grid=(8,),
            in_specs=[
                pl.BlockSpec((ROWS, WIDTH), lambda p, s: (0, 0)),
                pl.BlockSpec((1, WIDTH), lambda p, s: (0, 0)),
                pl.BlockSpec((1, 3, WIDTH, 128), lambda p, s: (p, 0, 0, 0)),
            ],
            out_specs=[
                pl.BlockSpec((1, 3, ROWS, 128), lambda p, s: (p, 0, 0, 0)),
                pl.BlockSpec((2, 192, 128), lambda p, s: (p, 0, 0)),
            ],
            scratch_shapes=[pltpu.VMEM((ROWS, WIDTH), BF), pltpu.VMEM((3, ROWS, 128), F32)],
        ),
        out_shape=[
            jax.ShapeDtypeStruct((8, 3, ROWS, 128), BF),
            jax.ShapeDtypeStruct((16, 192, 128), BF),
        ],
        name="project",
    )(scalars, rows, gain, weights)


def attend(score, values_t, scores, weights, bonus=()):
    blocks = scores.shape[0] // 256
    m = None
    for c in range(blocks):
        s = score(c)
        scores[256 * c : 256 * c + 256] = s
        part = jnp.max(s.reshape(32, 8, s.shape[1]), axis=0)
        m = part if m is None else jnp.maximum(m, part)
    m = jnp.max(m, axis=0, keepdims=True)
    for c in range(blocks):
        shift = m - (1.0 if c in bonus else 0.0)
        block = slice(256 * c, 256 * c + 256)
        weights[block] = jnp.exp2(scores[block] - shift).astype(BF)
    return jnp.dot(values_t, weights[...], preferred_element_type=F32), m


def near_kernel(s_ref, x_ref, gain_ref, w_ref, own_ref, out_ref, normed, keys, scores, weights):
    p = pl.program_id(0)

    @pl.when(p == 0)
    def _():
        normed[...] = norm_rows(x_ref[...].astype(F32), gain_ref[...]).astype(BF)

    rows = normed[...]
    k = jnp.dot(rows, w_ref[0, 0], preferred_element_type=F32).astype(BF).astype(F32)
    v = jnp.dot(rows, w_ref[0, 1], preferred_element_type=F32).astype(BF).astype(F32)
    partner = s_ref[1] + 1 - 2 * (s_ref[1] % 2)
    k, v = mask_key_value(k, v, partner * ROWS, s_ref[0])
    keys[:ROWS] = own_ref[0, 0]
    keys[ROWS:] = k.astype(BF)
    values_t = jnp.concatenate([own_ref[0, 1], v.astype(BF)], axis=0).T
    queries = own_ref[0, 2]
    for a in range(2):
        part = jnp.where(lanes(queries.shape) // WIDE == a, queries, jnp.zeros_like(queries))
        numer, m = attend(
            lambda i: nt(keys[256 * i : 256 * i + 256], part),
            values_t[a * WIDE : (a + 1) * WIDE],
            scores.at[a],
            weights.at[a],
        )
        row = lax.broadcasted_iota(jnp.int32, numer.shape, 0)
        out_ref[a] = jnp.where(row == HEAD + 1, m, numer)


def near(scalars, rows, gain, weights, own, first, count):
    return pl.pallas_call(
        near_kernel,
        grid_spec=pltpu.PrefetchScalarGridSpec(
            num_scalar_prefetch=1,
            grid=(count,),
            in_specs=[
                pl.BlockSpec((ROWS, WIDTH), lambda p, s: (0, 0)),
                pl.BlockSpec((1, WIDTH), lambda p, s: (0, 0)),
                pl.BlockSpec((1, 2, WIDTH, 128), lambda p, s: (p + first, 0, 0, 0)),
                pl.BlockSpec((1, 3, ROWS, 128), lambda p, s: (p + first, 0, 0, 0)),
            ],
            out_specs=pl.BlockSpec((2, WIDE, ROWS), lambda p, s: (p, 0, 0)),
            scratch_shapes=[
                pltpu.VMEM((ROWS, WIDTH), BF),
                pltpu.VMEM((2 * ROWS, 128), BF),
                pltpu.VMEM((2, 2 * ROWS, ROWS), F32),
                pltpu.VMEM((2, 2 * ROWS, ROWS), BF),
            ],
        ),
        out_shape=jax.ShapeDtypeStruct((2 * count, WIDE, ROWS), F32),
        cost_estimate=pl.CostEstimate(
            flops=5_000_000_000 * count,
            bytes_accessed=1_000_000 * count,
            transcendentals=1_050_000 * count,
        ),
        name="near",
    )(scalars, rows, gain, weights, own)


def to_lse(numer, m):
    total = numer[HEAD : HEAD + 1]
    lse = jnp.where(total > 0.0, m + jnp.log2(jnp.maximum(total, 1.0)), NEGATIVE)
    return numer / jnp.maximum(total, 1.0), lse


def packed_result(numer, m):
    mean, lse = to_lse(numer, m)
    high = lse.astype(BF).astype(F32)
    rest = lse - high
    second = rest.astype(BF).astype(F32)
    third = rest - second
    row = lax.broadcasted_iota(jnp.int32, mean.shape, 0)
    out = jnp.where(row < HEAD, mean, 0.0)
    out = jnp.where(row == HEAD, high, out)
    out = jnp.where(row == HEAD + 1, second, out)
    return jnp.where(row == HEAD + 2, third, out)


def middle_kernel(s_ref, in_ref, out_ref, keys_t, values_t, queries_t, keys, scores, weights):
    off4 = s_ref[2 + s_ref[1] % HEADS] % 4
    row = lax.broadcasted_iota(jnp.int32, (WIDE - HEAD, 1024), 0)
    first = row == 0
    for g in range(2):
        base = g * WIDE
        for i in range(8):
            part = slice(i * 128, (i + 1) * 128)
            for j, ref in enumerate((keys_t, values_t, queries_t)):
                ref[base : base + HEAD, part] = in_ref[8 * g + i, HEAD * (j + 1) : HEAD * (j + 2)]
        start = (s_ref[1] // HEADS * 2 + g) * 4096 + off4
        alive = start + 4 * lanes(row.shape) < s_ref[0]
        spare = slice(base + HEAD, base + WIDE)
        keys_t[spare] = jnp.where(first & (~alive), NEGATIVE, 0.0).astype(BF)
        values_t[spare] = jnp.where(first & alive, 1.0, 0.0).astype(BF)
        queries_t[spare] = jnp.where(first, 1.0, 0.0).astype(BF)
        alive = start + 4 * lanes((HEAD, 1024)) < s_ref[0]
        values = values_t[base : base + HEAD]
        values_t[base : base + HEAD] = jnp.where(alive, values, jnp.zeros_like(values))
    keys[...] = keys_t[...].T
    for c in range(0, 1024, 512):
        queries = queries_t[:, c : c + 512]
        owner = lax.broadcasted_iota(jnp.int32, queries.shape, 0) // WIDE
        for g in range(2):
            part = jnp.where(owner == g, queries, jnp.zeros_like(queries))
            numer, m = attend(
                lambda i: jnp.dot(
                    keys[256 * i : 256 * i + 256], part, preferred_element_type=F32
                ),
                values_t[g * WIDE : (g + 1) * WIDE],
                scores.at[g],
                weights.at[g],
            )
            out = packed_result(numer, m).astype(BF)
            for i in range(4):
                out_ref[8 * g + c // 128 + i] = out[:, i * 128 : (i + 1) * 128]


def middle(scalars, received):
    return pl.pallas_call(
        middle_kernel,
        grid_spec=pltpu.PrefetchScalarGridSpec(
            num_scalar_prefetch=1,
            grid=(1,),
            in_specs=[pl.BlockSpec((16, 192, 128), lambda i, s: (0, 0, 0))],
            out_specs=pl.BlockSpec((16, WIDE, 128), lambda i, s: (0, 0, 0)),
            scratch_shapes=[pltpu.VMEM((128, 1024), BF)] * 3
            + [
                pltpu.VMEM((1024, 128), BF),
                pltpu.VMEM((2, 1024, 512), F32),
                pltpu.VMEM((2, 1024, 512), BF),
            ],
        ),
        out_shape=jax.ShapeDtypeStruct((16, WIDE, 128), BF),
        cost_estimate=pl.CostEstimate(
            flops=10_000_000_000, bytes_accessed=1_000_000, transcendentals=2_100_000
        ),
        name="middle",
    )(scalars, received)


def far_kernel(own_ref, *refs):
    key_refs = (own_ref,) + refs[:3]
    in_ref, mid_ref, out_ref, scores, weights, values_t = refs[3:]
    for c in range(8):
        block = key_refs[c // 2][16 * (c % 2) : 16 * (c % 2) + 16].reshape(512, 128)
        values_t[:, 512 * c : 512 * c + 512] = block.T[WIDE:]
    packed = in_ref[:, 32:48].reshape(256, 128).astype(F32)
    queries = jnp.concatenate([packed, pltpu.roll(packed, WIDE, 1)], axis=0)
    queries = jnp.where(lanes(queries.shape) < WIDE, queries, 0.0).astype(BF)

    def score(c):
        block = key_refs[c // 4][8 * (c % 4) : 8 * (c % 4) + 8]
        return nt(block.reshape(256, 128), queries)

    numer, m = attend(score, values_t[...], scores, weights, range(4))
    out = packed_result(numer, m)
    out = jnp.concatenate([out, jnp.zeros_like(out)], axis=0).T.astype(BF)
    for half in range(2):
        part = out[256 * half : 256 * half + 256]
        out_ref[:, 16 * half : 16 * half + 16] = part.reshape(16, 16, 128)
    out_ref[:, 32:] = mid_ref[...]


def far(keys, received, mid_result):
    return pl.pallas_call(
        far_kernel,
        out_shape=jax.ShapeDtypeStruct((16, 96, 128), BF),
        scratch_shapes=[
            pltpu.VMEM((4096, 512), F32),
            pltpu.VMEM((4096, 512), BF),
            pltpu.VMEM((WIDE, 4096), BF),
        ],
        cost_estimate=pl.CostEstimate(
            flops=10_000_000_000, bytes_accessed=1_000_000, transcendentals=2_100_000
        ),
        name="far",
    )(*keys, received, mid_result)


def finish_kernel(s_ref, near0_ref, near1_ref, near2_ref, in_ref, x_ref, gain_ref, w_ref, out_ref, mixed):
    lane = lanes((1, ROWS))
    column4 = lanes((128, ROWS)) - 4 * lax.broadcasted_iota(jnp.int32, (128, ROWS), 0)
    column16 = lanes((32, ROWS)) - 16 * lax.broadcasted_iota(jnp.int32, (32, ROWS), 0)
    for h in range(HEADS):
        off = s_ref[2 + h]
        off4 = off % 4
        off16 = off % 16
        near_ref, i = ((near0_ref, h), (near1_ref, h - 8), (near2_ref, h - 12))[max(h // 4 - 1, 0)]
        mean_n, lse_n = to_lse(near_ref[i], near_ref[i, HEAD + 1 : HEAD + 2])
        spread4 = jnp.where(column4 == off4, 1.0, 0.0).astype(BF)
        mid = jnp.dot(
            in_ref[h, 32:], spread4, preferred_element_type=F32
        )
        spread16 = jnp.where(column16 == off16, 1.0, 0.0).astype(BF)
        distant = lax.dot_general(
            in_ref[h, :32], spread16, (((0,), (0,)), ((), ())), preferred_element_type=F32
        )

        def lse_of(spread):
            lse = spread[HEAD : HEAD + 1] + spread[HEAD + 1 : HEAD + 2]
            return lse + spread[HEAD + 2 : HEAD + 3]

        lse_m = jnp.where(lane % 4 == off4, lse_of(mid), NEGATIVE)
        lse_f = jnp.where(lane % 16 == off16, lse_of(distant), NEGATIVE)
        top = jnp.maximum(jnp.maximum(lse_n, lse_m), lse_f)
        weight_n = jnp.exp2(lse_n - top)
        weight_m = jnp.exp2(lse_m - top)
        weight_f = jnp.exp2(lse_f - top)
        inverse = 1.0 / jnp.maximum(weight_n + weight_m + weight_f, 1.0)
        mixed[HEAD * h : HEAD * (h + 1)] = (
            mean_n[:HEAD] * (weight_n * inverse)
            + mid[:HEAD] * (weight_m * inverse)
            + distant[:HEAD] * (weight_f * inverse)
        ).astype(BF)
    attended = mixed[...].T.astype(F32)
    sub = norm_rows(attended, gain_ref[...]).astype(BF)
    out = x_ref[...].astype(F32) + jnp.dot(sub, w_ref[...], preferred_element_type=F32)
    out_ref[...] = out.astype(BF)


def finish(scalars, near_results, dilated, rows, gain, w_out):
    def whole(*shape):
        return pl.BlockSpec(shape, lambda i, s: (0,) * len(shape))

    return pl.pallas_call(
        finish_kernel,
        grid_spec=pltpu.PrefetchScalarGridSpec(
            num_scalar_prefetch=1,
            grid=(1,),
            in_specs=[
                whole(8, WIDE, ROWS),
                whole(4, WIDE, ROWS),
                whole(4, WIDE, ROWS),
                whole(16, 96, 128),
                whole(ROWS, WIDTH),
                whole(1, WIDTH),
                whole(WIDTH, WIDTH),
            ],
            out_specs=whole(ROWS, WIDTH),
            scratch_shapes=[pltpu.VMEM((WIDTH, ROWS), BF)],
        ),
        out_shape=jax.ShapeDtypeStruct((ROWS, WIDTH), BF),
        name="finish",
    )(scalars, *near_results, dilated, rows, gain, w_out)


def exchange(value, axis):
    return lax.all_to_all(value, axis, split_axis=0, concat_axis=0, tiled=True)


def body(tile_embed, valid_tiles, offsets, norm_gain, w_qkv, sub_gain, w_out):
    position = lax.axis_index(("y", "xh", "xl", "z"))
    scalars = jnp.concatenate([valid_tiles, position.astype(jnp.int32)[None], offsets])
    arrived = exchange(tile_embed.reshape(128, 4, WIDTH), ("y", "xh", "xl", "z"))
    rows = arrived.transpose(1, 0, 2).reshape(ROWS, WIDTH)
    partner = lax.ppermute(rows, "z", [(i, i ^ 1) for i in range(8)])
    weights = widen(w_qkv)
    gain = norm_gain[None]
    own, send = project(scalars, rows, gain, weights)
    received = exchange(send, ("xl", "z"))
    mine = received[:, :32]
    other = lax.ppermute(mine, "xh", [(0, 1), (1, 0)])
    keys = [jnp.concatenate([mine, other])]
    for y in range(1, 4):
        keys.append(lax.ppermute(keys[0], "y", [(i, (i + y) % 4) for i in range(4)]))
    near_results = []
    for first, count in ((0, 4), (4, 2), (6, 2)):
        near_results.append(near(scalars, partner, gain, weights, own, first, count))
    mid_result = middle(scalars, received)
    far_result = far(keys, received, mid_result)
    dilated = exchange(far_result, ("xl", "z"))
    return finish(scalars, near_results, dilated, rows, sub_gain[None], w_out)


def solution(mesh):
    inner = Mesh(mesh.devices.reshape(4, 2, 2, 8, 2), ("y", "xh", "xl", "z", "slide"))
    split = P(("slide", "y", "xh", "xl", "z"), None)
    return jax.shard_map(
        body,
        mesh=inner,
        in_specs=(split, P("slide"), P(), P(), P(), P(), P()),
        out_specs=split,
        check_vma=False,
    )
```

```python
import math

import jax
import jax.numpy as jnp
from jax import lax
from jax.experimental import pallas as pl
from jax.experimental.pallas import tpu as pltpu
from jax.sharding import Mesh, PartitionSpec as P


HEADS = 16
HEAD = 48
WIDE = 64
ROWS = 512
WIDTH = 768
NEGATIVE = -1e30
EPSILON = 1e-05
SCALE = math.log2(math.e) / math.sqrt(HEAD)
BF = jnp.bfloat16
F32 = jnp.float32


def norm_rows(x, gain):
    mean = jnp.mean(x, axis=-1, keepdims=True)
    centred = x - mean
    var = jnp.mean(centred * centred, axis=-1, keepdims=True)
    return centred * lax.rsqrt(var + EPSILON) * gain


def lanes(shape):
    return lax.broadcasted_iota(jnp.int32, shape, len(shape) - 1)


def mask_key_value(k, v, first, valid):
    lane = lanes(k.shape)
    special = lane % WIDE == HEAD
    alive = first + lax.broadcasted_iota(jnp.int32, k.shape, 0) < valid
    k = jnp.where(special, jnp.where(alive, 0.0, NEGATIVE), k)
    v = jnp.where(alive, jnp.where(special, 1.0, v), 0.0)
    return k, v


def nt(a, b):
    return lax.dot_general(a, b, (((1,), (1,)), ((), ())), preferred_element_type=F32)


def widen_kernel(w_ref, out_ref):
    for j, start in enumerate((WIDTH, 2 * WIDTH, 0)):
        for p in range(8):
            first = start + 2 * HEAD * p
            window = first // 128 * 128
            row = lax.broadcasted_iota(jnp.int32, (256, 128), 0) + (window - first)
            lane = lanes((256, 128))
            column = lane % WIDE + lane // WIDE * HEAD
            chosen = (row == column) & (lane % WIDE < HEAD)
            pick = jnp.where(chosen, 1.0, 0.0).astype(BF)
            wide = min(256, 3 * WIDTH - window)
            part = jnp.dot(
                w_ref[:, window : window + wide], pick[:wide], preferred_element_type=F32
            )
            out_ref[p, j] = part.astype(BF)


def widen(w_qkv):
    return pl.pallas_call(
        widen_kernel,
        out_shape=jax.ShapeDtypeStruct((8, 3, WIDTH, 128), BF),
        cost_estimate=pl.CostEstimate(
            flops=10_000_000_000, bytes_accessed=8_000_000, transcendentals=0
        ),
        name="widen",
    )(w_qkv)


def project_kernel(s_ref, x_ref, gain_ref, w_ref, own_ref, send_ref, normed, stage):
    p = pl.program_id(0)

    @pl.when(p == 0)
    def _():
        normed[...] = norm_rows(x_ref[...].astype(F32), gain_ref[...]).astype(BF)

    rows = normed[...]
    for u in range(2):
        k = jnp.dot(rows, w_ref[u, 0], preferred_element_type=F32).astype(BF).astype(F32)
        v = jnp.dot(rows, w_ref[u, 1], preferred_element_type=F32).astype(BF).astype(F32)
        q = jnp.dot(rows, w_ref[u, 2], preferred_element_type=F32).astype(BF).astype(F32)
        k, v = mask_key_value(k, v, s_ref[1] * ROWS, s_ref[0])
        q = jnp.where(lanes(q.shape) % WIDE == HEAD, 1.0, q)
        stage[u, 0] = k
        stage[u, 1] = v
        stage[u, 2] = q
        own_ref[u, 0] = k.astype(BF)
        own_ref[u, 1] = v.astype(BF)
        own_ref[u, 2] = q.astype(BF)
        low = lanes((ROWS // 4, 128)) < WIDE
        off = [s_ref[2 + 4 * p + 2 * u + a] for a in range(2)]
        for j in range(3):
            first = stage[u, j, pl.ds(off[0] % 4, ROWS // 4, stride=4), :]
            second = stage[u, j, pl.ds(off[1] % 4, ROWS // 4, stride=4), :]
            chosen = jnp.where(low, first, second).astype(BF).T
            for a in range(2):
                send_ref[2 * u + a, HEAD * (j + 1) : HEAD * (j + 2)] = chosen[a * WIDE : a * WIDE + HEAD]
        low = lanes((ROWS // 16, 128)) < WIDE
        for a in range(2):
            k, v, q = [stage[u, j, pl.ds(off[a] % 16, ROWS // 16, stride=16), :] for j in range(3)]
            if a == 0:
                v = pltpu.roll(v, WIDE, 1)
                q_high = pltpu.roll(q, WIDE, 1)
            else:
                k = pltpu.roll(k, WIDE, 1)
                q_high = q
                q = pltpu.roll(q, WIDE, 1)
            send_ref[2 * u + a, :32] = jnp.where(low, k, v).astype(BF)
            send_ref[2 * u + a, 32:48] = jnp.where(low[:16], q[:16], q_high[16:]).astype(BF)


def project(scalars, rows, gain, weights):
    return pl.pallas_call(
        project_kernel,
        grid_spec=pltpu.PrefetchScalarGridSpec(
            num_scalar_prefetch=1,
            grid=(4,),
            in_specs=[
                pl.BlockSpec((ROWS, WIDTH), lambda p, s: (0, 0)),
                pl.BlockSpec((1, WIDTH), lambda p, s: (0, 0)),
                pl.BlockSpec((2, 3, WIDTH, 128), lambda p, s: (p, 0, 0, 0)),
            ],
            out_specs=[
                pl.BlockSpec((2, 3, ROWS, 128), lambda p, s: (p, 0, 0, 0)),
                pl.BlockSpec((4, 192, 128), lambda p, s: (p, 0, 0)),
            ],
            scratch_shapes=[pltpu.VMEM((ROWS, WIDTH), BF), pltpu.VMEM((2, 3, ROWS, 128), F32)],
        ),
        out_shape=[
            jax.ShapeDtypeStruct((8, 3, ROWS, 128), BF),
            jax.ShapeDtypeStruct((16, 192, 128), BF),
        ],
        name="project",
    )(scalars, rows, gain, weights)


def attend(score, values_t, scores, weights, bonus=()):
    return attend_all([(score, values_t, scores, weights, bonus)])[0]


def attend_all(streams):
    results = []
    tops = [None] * len(streams)

    def score_block(n, c):
        score, _, scores, _, _ = streams[n]
        s = score(c) * SCALE
        scores[256 * c : 256 * c + 256] = s
        part = jnp.max(s.reshape(32, 8, s.shape[1]), axis=0)
        tops[n] = part if tops[n] is None else jnp.maximum(tops[n], part)

    for c in range(streams[0][2].shape[0] // 256):
        score_block(0, c)
    for n, (_, values_t, scores, weights, bonus) in enumerate(streams):
        m = jnp.max(tops[n], axis=0, keepdims=True)
        for c in range(scores.shape[0] // 256):
            if n + 1 < len(streams):
                score_block(n + 1, c)
            shift = m - (1.0 if c in bonus else 0.0)
            block = slice(256 * c, 256 * c + 256)
            weights[block] = jnp.exp2(scores[block] - shift).astype(BF)
        results.append((jnp.dot(values_t, weights[...], preferred_element_type=F32), m))
    return results


def near_kernel(s_ref, x_ref, gain_ref, w_ref, own_ref, out_ref, normed, keys, scores, weights):
    p = pl.program_id(0)

    @pl.when(p == 0)
    def _():
        normed[...] = norm_rows(x_ref[...].astype(F32), gain_ref[...]).astype(BF)

    rows = normed[...]
    k = jnp.dot(rows, w_ref[0, 0], preferred_element_type=F32).astype(BF).astype(F32)
    v = jnp.dot(rows, w_ref[0, 1], preferred_element_type=F32).astype(BF).astype(F32)
    partner = s_ref[1] + 1 - 2 * (s_ref[1] % 2)
    k, v = mask_key_value(k, v, partner * ROWS, s_ref[0])
    keys[:ROWS] = own_ref[0, 0]
    keys[ROWS:] = k.astype(BF)
    values_t = jnp.concatenate([own_ref[0, 1], v.astype(BF)], axis=0).T
    queries = own_ref[0, 2]
    streams = []
    for a in range(2):
        part = jnp.where(lanes(queries.shape) // WIDE == a, queries, jnp.zeros_like(queries))
        streams.append(
            (
                lambda i, part=part: nt(keys[256 * i : 256 * i + 256], part),
                values_t[a * WIDE : (a + 1) * WIDE],
                scores.at[a],
                weights.at[a],
                (),
            )
        )
    for a, (numer, m) in enumerate(attend_all(streams)):
        row = lax.broadcasted_iota(jnp.int32, numer.shape, 0)
        out_ref[a] = jnp.where(row == HEAD + 1, m, numer)


def near(scalars, rows, gain, weights, own, first, count):
    return pl.pallas_call(
        near_kernel,
        grid_spec=pltpu.PrefetchScalarGridSpec(
            num_scalar_prefetch=1,
            grid=(count,),
            in_specs=[
                pl.BlockSpec((ROWS, WIDTH), lambda p, s: (0, 0)),
                pl.BlockSpec((1, WIDTH), lambda p, s: (0, 0)),
                pl.BlockSpec((1, 2, WIDTH, 128), lambda p, s: (p + first, 0, 0, 0)),
                pl.BlockSpec((1, 3, ROWS, 128), lambda p, s: (p + first, 0, 0, 0)),
            ],
            out_specs=pl.BlockSpec((2, WIDE, ROWS), lambda p, s: (p, 0, 0)),
            scratch_shapes=[
                pltpu.VMEM((ROWS, WIDTH), BF),
                pltpu.VMEM((2 * ROWS, 128), BF),
                pltpu.VMEM((2, 2 * ROWS, ROWS), F32),
                pltpu.VMEM((2, 2 * ROWS, ROWS), BF),
            ],
        ),
        out_shape=jax.ShapeDtypeStruct((2 * count, WIDE, ROWS), F32),
        cost_estimate=pl.CostEstimate(
            flops=5_000_000_000 * count,
            bytes_accessed=1_000_000 * count,
            transcendentals=1_050_000 * count,
        ),
        name="near",
    )(scalars, rows, gain, weights, own)


def to_lse(numer, m):
    total = numer[HEAD : HEAD + 1]
    lse = jnp.where(total > 0.0, m + jnp.log2(jnp.maximum(total, 1.0)), NEGATIVE)
    return numer / jnp.maximum(total, 1.0), lse


def packed_result(numer, m):
    mean, lse = to_lse(numer, m)
    high = lse.astype(BF).astype(F32)
    rest = lse - high
    second = rest.astype(BF).astype(F32)
    third = rest - second
    row = lax.broadcasted_iota(jnp.int32, mean.shape, 0)
    out = jnp.where(row < HEAD, mean, 0.0)
    out = jnp.where(row == HEAD, high, out)
    out = jnp.where(row == HEAD + 1, second, out)
    return jnp.where(row == HEAD + 2, third, out)


def middle_kernel(s_ref, in_ref, out_ref, keys_t, values_t, queries_t, keys, scores, weights):
    off4 = s_ref[2 + s_ref[1] % HEADS] % 4
    row = lax.broadcasted_iota(jnp.int32, (WIDE - HEAD, 1024), 0)
    first = row == 0
    for g in range(2):
        base = g * WIDE
        for i in range(8):
            part = slice(i * 128, (i + 1) * 128)
            for j, ref in enumerate((keys_t, values_t, queries_t)):
                ref[base : base + HEAD, part] = in_ref[8 * g + i, HEAD * (j + 1) : HEAD * (j + 2)]
        start = (s_ref[1] // HEADS * 2 + g) * 4096 + off4
        alive = start + 4 * lanes(row.shape) < s_ref[0]
        spare = slice(base + HEAD, base + WIDE)
        keys_t[spare] = jnp.where(first & (~alive), NEGATIVE, 0.0).astype(BF)
        values_t[spare] = jnp.where(first & alive, 1.0, 0.0).astype(BF)
        queries_t[spare] = jnp.where(first, 1.0, 0.0).astype(BF)
        alive = start + 4 * lanes((HEAD, 1024)) < s_ref[0]
        values = values_t[base : base + HEAD]
        values_t[base : base + HEAD] = jnp.where(alive, values, jnp.zeros_like(values))
    keys[...] = keys_t[...].T
    for c in range(0, 1024, 512):
        queries = queries_t[:, c : c + 512]
        owner = lax.broadcasted_iota(jnp.int32, queries.shape, 0) // WIDE
        for g in range(2):
            part = jnp.where(owner == g, queries, jnp.zeros_like(queries))
            numer, m = attend(
                lambda i: jnp.dot(
                    keys[256 * i : 256 * i + 256], part, preferred_element_type=F32
                ),
                values_t[g * WIDE : (g + 1) * WIDE],
                scores.at[g],
                weights.at[g],
            )
            out = packed_result(numer, m).astype(BF)
            for i in range(4):
                out_ref[8 * g + c // 128 + i] = out[:, i * 128 : (i + 1) * 128]


def middle(scalars, received):
    return pl.pallas_call(
        middle_kernel,
        grid_spec=pltpu.PrefetchScalarGridSpec(
            num_scalar_prefetch=1,
            grid=(1,),
            in_specs=[pl.BlockSpec((16, 192, 128), lambda i, s: (0, 0, 0))],
            out_specs=pl.BlockSpec((16, WIDE, 128), lambda i, s: (0, 0, 0)),
            scratch_shapes=[pltpu.VMEM((128, 1024), BF)] * 3
            + [
                pltpu.VMEM((1024, 128), BF),
                pltpu.VMEM((2, 1024, 512), F32),
                pltpu.VMEM((2, 1024, 512), BF),
            ],
        ),
        out_shape=jax.ShapeDtypeStruct((16, WIDE, 128), BF),
        cost_estimate=pl.CostEstimate(
            flops=10_000_000_000, bytes_accessed=1_000_000, transcendentals=2_100_000
        ),
        name="middle",
    )(scalars, received)


def far_kernel(own_ref, *refs):
    key_refs = (own_ref,) + refs[:3]
    in_ref, mid_ref, out_ref, scores, weights, values_t = refs[3:]
    for c in range(8):
        block = key_refs[c // 2][16 * (c % 2) : 16 * (c % 2) + 16].reshape(512, 128)
        values_t[:, 512 * c : 512 * c + 512] = block.T[WIDE:]
    packed = in_ref[:, 32:48].reshape(256, 128).astype(F32)
    queries = jnp.concatenate([packed, pltpu.roll(packed, WIDE, 1)], axis=0)
    queries = jnp.where(lanes(queries.shape) < WIDE, queries, 0.0).astype(BF)

    def score(c):
        block = key_refs[c // 4][8 * (c % 4) : 8 * (c % 4) + 8]
        return nt(block.reshape(256, 128), queries)

    numer, m = attend(score, values_t[...], scores, weights, range(4))
    out = packed_result(numer, m)
    out = jnp.concatenate([out[:, :256], out[:, 256:]], axis=0).T.astype(BF)
    out_ref[:, :16] = out.reshape(16, 16, 128)
    out_ref[:, 16:] = mid_ref[:, :56]


def far(keys, received, mid_result):
    return pl.pallas_call(
        far_kernel,
        out_shape=jax.ShapeDtypeStruct((16, 72, 128), BF),
        scratch_shapes=[
            pltpu.VMEM((4096, 512), F32),
            pltpu.VMEM((4096, 512), BF),
            pltpu.VMEM((WIDE, 4096), BF),
        ],
        cost_estimate=pl.CostEstimate(
            flops=10_000_000_000, bytes_accessed=1_000_000, transcendentals=2_100_000
        ),
        name="far",
    )(*keys, received, mid_result)


def finish_kernel(s_ref, near0_ref, near1_ref, near2_ref, in_ref, x_ref, gain_ref, w_ref, out_ref, mixed):
    lane = lanes((1, ROWS))
    column4 = lanes((128, ROWS)) - 4 * lax.broadcasted_iota(jnp.int32, (128, ROWS), 0)
    column16 = lanes((16, 256)) - 16 * lax.broadcasted_iota(jnp.int32, (16, 256), 0)
    for h in range(HEADS):
        off = s_ref[2 + h]
        off4 = off % 4
        off16 = off % 16
        near_ref = near0_ref if h < 10 else near1_ref if h < 14 else near2_ref
        i = h if h < 10 else h - 10 if h < 14 else h - 14
        mean_n, lse_n = to_lse(near_ref[i], near_ref[i, HEAD + 1 : HEAD + 2])
        spread4 = jnp.where(column4 == off4, 1.0, 0.0).astype(BF)
        mid = jnp.dot(
            in_ref[h, 16:], spread4, preferred_element_type=F32
        )
        spread16 = jnp.where(column16 == off16, 1.0, 0.0).astype(BF)
        distant = lax.dot_general(
            in_ref[h, :16], spread16, (((0,), (0,)), ((), ())), preferred_element_type=F32
        )
        distant = jnp.concatenate([distant[:WIDE], distant[WIDE:]], axis=1)

        def lse_of(spread):
            lse = spread[HEAD : HEAD + 1] + spread[HEAD + 1 : HEAD + 2]
            return lse + spread[HEAD + 2 : HEAD + 3]

        lse_m = jnp.where(lane % 4 == off4, lse_of(mid), NEGATIVE)
        lse_f = jnp.where(lane % 16 == off16, lse_of(distant), NEGATIVE)
        top = jnp.maximum(jnp.maximum(lse_n, lse_m), lse_f)
        weight_n = jnp.exp2(lse_n - top)
        weight_m = jnp.exp2(lse_m - top)
        weight_f = jnp.exp2(lse_f - top)
        inverse = 1.0 / jnp.maximum(weight_n + weight_m + weight_f, 1.0)
        mixed[HEAD * h : HEAD * (h + 1)] = (
            mean_n[:HEAD] * (weight_n * inverse)
            + mid[:HEAD] * (weight_m * inverse)
            + distant[:HEAD] * (weight_f * inverse)
        ).astype(BF)
    attended = mixed[...].T.astype(F32)
    sub = norm_rows(attended, gain_ref[...]).astype(BF)
    out = x_ref[...].astype(F32) + jnp.dot(sub, w_ref[...], preferred_element_type=F32)
    out_ref[...] = out.astype(BF)


def finish(scalars, near_results, dilated, rows, gain, w_out):
    def whole(*shape):
        return pl.BlockSpec(shape, lambda i, s: (0,) * len(shape))

    return pl.pallas_call(
        finish_kernel,
        grid_spec=pltpu.PrefetchScalarGridSpec(
            num_scalar_prefetch=1,
            grid=(1,),
            in_specs=[
                whole(10, WIDE, ROWS),
                whole(4, WIDE, ROWS),
                whole(2, WIDE, ROWS),
                whole(16, 72, 128),
                whole(ROWS, WIDTH),
                whole(1, WIDTH),
                whole(WIDTH, WIDTH),
            ],
            out_specs=whole(ROWS, WIDTH),
            scratch_shapes=[pltpu.VMEM((WIDTH, ROWS), BF)],
        ),
        out_shape=jax.ShapeDtypeStruct((ROWS, WIDTH), BF),
        name="finish",
    )(scalars, *near_results, dilated, rows, gain, w_out)


def exchange(value, axis):
    return lax.all_to_all(value, axis, split_axis=0, concat_axis=0, tiled=True)


def body(tile_embed, valid_tiles, offsets, norm_gain, w_qkv, sub_gain, w_out):
    position = lax.axis_index(("y", "xh", "xl", "z"))
    scalars = jnp.concatenate([valid_tiles, position.astype(jnp.int32)[None], offsets])
    gain, last_gain = norm_gain[None], sub_gain[None]
    arrived = exchange(tile_embed.reshape(128, 4, WIDTH), ("y", "xh", "xl", "z"))
    rows = arrived.transpose(1, 0, 2).reshape(ROWS, WIDTH)
    partner = lax.ppermute(rows, "z", [(i, i ^ 1) for i in range(8)])
    weights = widen(w_qkv)
    own, send = project(scalars, rows, gain, weights)
    received = exchange(send, ("xl", "z"))
    mine = received[:, :32]
    other = lax.ppermute(mine, "xh", [(0, 1), (1, 0)])
    keys = [jnp.concatenate([mine, other])]
    for y in range(1, 4):
        keys.append(lax.ppermute(keys[0], "y", [(i, (i + y) % 4) for i in range(4)]))
    near_results = []
    for first, count in ((0, 5), (5, 2), (7, 1)):
        near_results.append(near(scalars, partner, gain, weights, own, first, count))
    mid_result = middle(scalars, received)
    far_result = far(keys, received, mid_result)
    dilated = exchange(far_result, ("xl", "z"))
    return finish(scalars, near_results, dilated, rows, last_gain, w_out)


def solution(mesh):
    inner = Mesh(mesh.devices.reshape(4, 2, 2, 8, 2), ("y", "xh", "xl", "z", "slide"))
    split = P(("slide", "y", "xh", "xl", "z"), None)
    return jax.shard_map(
        body,
        mesh=inner,
        in_specs=(split, P("slide"), P(), P(), P(), P(), P()),
        out_specs=split,
        check_vma=False,
    )
```

```python
import math

import jax
import jax.numpy as jnp
from jax import lax
from jax.experimental import pallas as pl
from jax.experimental.pallas import tpu as pltpu
from jax.sharding import Mesh, PartitionSpec as P


HEADS = 16
HEAD = 48
WIDE = 64
ROWS = 512
WIDTH = 768
NEGATIVE = -1e30
EPSILON = 1e-05
SCALE = math.log2(math.e) / math.sqrt(HEAD)
BF = jnp.bfloat16
F32 = jnp.float32


def norm_rows(x, gain):
    mean = jnp.mean(x, axis=-1, keepdims=True)
    centred = x - mean
    var = jnp.mean(centred * centred, axis=-1, keepdims=True)
    return centred * lax.rsqrt(var + EPSILON) * gain


def lanes(shape):
    return lax.broadcasted_iota(jnp.int32, shape, len(shape) - 1)


def mask_key_value(k, v, first, valid):
    lane = lanes(k.shape)
    special = lane % WIDE == HEAD
    alive = first + lax.broadcasted_iota(jnp.int32, k.shape, 0) < valid
    k = jnp.where(special, jnp.where(alive, 0.0, NEGATIVE), k)
    v = jnp.where(alive, jnp.where(special, 1.0, v), 0.0)
    return k, v


def nt(a, b):
    return lax.dot_general(a, b, (((1,), (1,)), ((), ())), preferred_element_type=F32)


def widen_kernel(w_ref, out_ref):
    for j, start in enumerate((WIDTH, 2 * WIDTH, 0)):
        for p in range(8):
            first = start + 2 * HEAD * p
            window = first // 128 * 128
            row = lax.broadcasted_iota(jnp.int32, (256, 128), 0) + (window - first)
            lane = lanes((256, 128))
            column = lane % WIDE + lane // WIDE * HEAD
            chosen = (row == column) & (lane % WIDE < HEAD)
            pick = jnp.where(chosen, 1.0, 0.0).astype(BF)
            wide = min(256, 3 * WIDTH - window)
            part = jnp.dot(
                w_ref[:, window : window + wide], pick[:wide], preferred_element_type=F32
            )
            column = 512 + 128 * (p % 2) if j == 2 else 256 * (p % 2) + 128 * j
            out_ref[p // 2, :, column : column + 128] = part.astype(BF)


def widen(w_qkv):
    return pl.pallas_call(
        widen_kernel,
        out_shape=jax.ShapeDtypeStruct((4, WIDTH, WIDTH), BF),
        cost_estimate=pl.CostEstimate(
            flops=10_000_000_000, bytes_accessed=8_000_000, transcendentals=0
        ),
        name="widen",
    )(w_qkv)


def project_kernel(s_ref, x_ref, gain_ref, w_ref, own_ref, send_ref, normed, stage):
    p = pl.program_id(0)

    @pl.when(p == 0)
    def _():
        normed[...] = norm_rows(x_ref[...].astype(F32), gain_ref[...]).astype(BF)

    rows = normed[...]
    projected = jnp.dot(rows, w_ref[0], preferred_element_type=F32)
    projected = projected.astype(BF).astype(F32)
    for u in range(2):
        k = projected[:, 256 * u : 256 * u + 128]
        v = projected[:, 256 * u + 128 : 256 * u + 256]
        q = projected[:, 512 + 128 * u : 640 + 128 * u]
        k, v = mask_key_value(k, v, s_ref[1] * ROWS, s_ref[0])
        q = jnp.where(lanes(q.shape) % WIDE == HEAD, 1.0, q)
        stage[u, 0] = k
        stage[u, 1] = v
        stage[u, 2] = q
        own_ref[u, 0] = k.astype(BF)
        own_ref[u, 1] = v.astype(BF)
        own_ref[u, 2] = q.astype(BF)
        low = lanes((ROWS // 4, 128)) < WIDE
        off = [s_ref[2 + 4 * p + 2 * u + a] for a in range(2)]
        for j in range(3):
            first = stage[u, j, pl.ds(off[0] % 4, ROWS // 4, stride=4), :]
            second = stage[u, j, pl.ds(off[1] % 4, ROWS // 4, stride=4), :]
            chosen = jnp.where(low, first, second).astype(BF).T
            for a in range(2):
                send_ref[2 * u + a, HEAD * (j + 1) : HEAD * (j + 2)] = chosen[a * WIDE : a * WIDE + HEAD]
        low = lanes((ROWS // 16, 128)) < WIDE
        for a in range(2):
            k, v, q = [stage[u, j, pl.ds(off[a] % 16, ROWS // 16, stride=16), :] for j in range(3)]
            if a == 0:
                v = pltpu.roll(v, WIDE, 1)
                q_high = pltpu.roll(q, WIDE, 1)
            else:
                k = pltpu.roll(k, WIDE, 1)
                q_high = q
                q = pltpu.roll(q, WIDE, 1)
            send_ref[2 * u + a, :32] = jnp.where(low, k, v).astype(BF)
            send_ref[2 * u + a, 32:48] = jnp.where(low[:16], q[:16], q_high[16:]).astype(BF)


def project(scalars, rows, gain, weights):
    return pl.pallas_call(
        project_kernel,
        grid_spec=pltpu.PrefetchScalarGridSpec(
            num_scalar_prefetch=1,
            grid=(4,),
            in_specs=[
                pl.BlockSpec((ROWS, WIDTH), lambda p, s: (0, 0)),
                pl.BlockSpec((1, WIDTH), lambda p, s: (0, 0)),
                pl.BlockSpec((1, WIDTH, WIDTH), lambda p, s: (p, 0, 0)),
            ],
            out_specs=[
                pl.BlockSpec((2, 3, ROWS, 128), lambda p, s: (p, 0, 0, 0)),
                pl.BlockSpec((4, 192, 128), lambda p, s: (p, 0, 0)),
            ],
            scratch_shapes=[pltpu.VMEM((ROWS, WIDTH), BF), pltpu.VMEM((2, 3, ROWS, 128), F32)],
        ),
        out_shape=[
            jax.ShapeDtypeStruct((8, 3, ROWS, 128), BF),
            jax.ShapeDtypeStruct((16, 192, 128), BF),
        ],
        name="project",
    )(scalars, rows, gain, weights)


def attend(score, values_t, scores, weights, bonus=()):
    return attend_all([(score, values_t, scores, weights, bonus)])[0]


def attend_all(streams):
    results = []
    tops = [None] * len(streams)

    def score_block(n, c):
        score, _, scores, _, _ = streams[n]
        s = score(c) * SCALE
        scores[256 * c : 256 * c + 256] = s
        part = jnp.max(s.reshape(32, 8, s.shape[1]), axis=0)
        tops[n] = part if tops[n] is None else jnp.maximum(tops[n], part)

    for c in range(streams[0][2].shape[0] // 256):
        score_block(0, c)
    for n, (_, values_t, scores, weights, bonus) in enumerate(streams):
        m = jnp.max(tops[n], axis=0, keepdims=True)
        for c in range(scores.shape[0] // 256):
            if n + 1 < len(streams):
                score_block(n + 1, c)
            shift = m - (1.0 if c in bonus else 0.0)
            block = slice(256 * c, 256 * c + 256)
            weights[block] = jnp.exp2(scores[block] - shift).astype(BF)
        results.append((jnp.dot(values_t, weights[...], preferred_element_type=F32), m))
    return results


def near_kernel(s_ref, x_ref, gain_ref, w_ref, own_ref, out_ref, normed, keys, scores, weights):
    p = pl.program_id(0)

    @pl.when(p == 0)
    def _():
        normed[...] = norm_rows(x_ref[...].astype(F32), gain_ref[...]).astype(BF)

    rows = normed[...]
    projected = jnp.dot(rows, w_ref[0], preferred_element_type=F32).astype(BF).astype(F32)
    k, v = projected[:, :128], projected[:, 128:]
    partner = s_ref[1] + 1 - 2 * (s_ref[1] % 2)
    k, v = mask_key_value(k, v, partner * ROWS, s_ref[0])
    keys[:ROWS] = own_ref[0, 0]
    keys[ROWS:] = k.astype(BF)
    values_t = jnp.concatenate([own_ref[0, 1], v.astype(BF)], axis=0).T
    queries = own_ref[0, 2]
    streams = []
    for a in range(2):
        part = jnp.where(lanes(queries.shape) // WIDE == a, queries, jnp.zeros_like(queries))
        streams.append(
            (
                lambda i, part=part: nt(keys[256 * i : 256 * i + 256], part),
                values_t[a * WIDE : (a + 1) * WIDE],
                scores.at[a],
                weights.at[a],
                (),
            )
        )
    for a, (numer, m) in enumerate(attend_all(streams)):
        row = lax.broadcasted_iota(jnp.int32, numer.shape, 0)
        out_ref[a] = jnp.where(row == HEAD + 1, m, numer)


def near(scalars, rows, gain, weights, own, first, count):
    return pl.pallas_call(
        near_kernel,
        grid_spec=pltpu.PrefetchScalarGridSpec(
            num_scalar_prefetch=1,
            grid=(count,),
            in_specs=[
                pl.BlockSpec((ROWS, WIDTH), lambda p, s: (0, 0)),
                pl.BlockSpec((1, WIDTH), lambda p, s: (0, 0)),
                pl.BlockSpec(
                    (1, WIDTH, 256), lambda p, s: ((p + first) // 2, 0, (p + first) % 2)
                ),
                pl.BlockSpec((1, 3, ROWS, 128), lambda p, s: (p + first, 0, 0, 0)),
            ],
            out_specs=pl.BlockSpec((2, WIDE, ROWS), lambda p, s: (p, 0, 0)),
            scratch_shapes=[
                pltpu.VMEM((ROWS, WIDTH), BF),
                pltpu.VMEM((2 * ROWS, 128), BF),
                pltpu.VMEM((2, 2 * ROWS, ROWS), F32),
                pltpu.VMEM((2, 2 * ROWS, ROWS), BF),
            ],
        ),
        out_shape=jax.ShapeDtypeStruct((2 * count, WIDE, ROWS), F32),
        cost_estimate=pl.CostEstimate(
            flops=5_000_000_000 * count,
            bytes_accessed=1_000_000 * count,
            transcendentals=1_050_000 * count,
        ),
        name="near",
    )(scalars, rows, gain, weights, own)


def to_lse(numer, m):
    total = numer[HEAD : HEAD + 1]
    lse = jnp.where(total > 0.0, m + jnp.log2(jnp.maximum(total, 1.0)), NEGATIVE)
    return numer / jnp.maximum(total, 1.0), lse


def packed_result(numer, m):
    mean, lse = to_lse(numer, m)
    high = lse.astype(BF).astype(F32)
    rest = lse - high
    second = rest.astype(BF).astype(F32)
    third = rest - second
    row = lax.broadcasted_iota(jnp.int32, mean.shape, 0)
    out = jnp.where(row < HEAD, mean, 0.0)
    out = jnp.where(row == HEAD, high, out)
    out = jnp.where(row == HEAD + 1, second, out)
    return jnp.where(row == HEAD + 2, third, out)


def middle_kernel(s_ref, in_ref, out_ref, keys_t, values_t, queries_t, keys, scores, weights):
    off4 = s_ref[2 + s_ref[1] % HEADS] % 4
    row = lax.broadcasted_iota(jnp.int32, (WIDE - HEAD, 1024), 0)
    first = row == 0
    for g in range(2):
        base = g * WIDE
        for i in range(8):
            part = slice(i * 128, (i + 1) * 128)
            for j, ref in enumerate((keys_t, values_t, queries_t)):
                ref[base : base + HEAD, part] = in_ref[8 * g + i, HEAD * (j + 1) : HEAD * (j + 2)]
        start = (s_ref[1] // HEADS * 2 + g) * 4096 + off4
        alive = start + 4 * lanes(row.shape) < s_ref[0]
        spare = slice(base + HEAD, base + WIDE)
        keys_t[spare] = jnp.where(first & (~alive), NEGATIVE, 0.0).astype(BF)
        values_t[spare] = jnp.where(first & alive, 1.0, 0.0).astype(BF)
        queries_t[spare] = jnp.where(first, 1.0, 0.0).astype(BF)
        alive = start + 4 * lanes((HEAD, 1024)) < s_ref[0]
        values = values_t[base : base + HEAD]
        values_t[base : base + HEAD] = jnp.where(alive, values, jnp.zeros_like(values))
    keys[...] = keys_t[...].T
    streams = []
    for c in range(0, 1024, 512):
        queries = queries_t[:, c : c + 512]
        owner = lax.broadcasted_iota(jnp.int32, queries.shape, 0) // WIDE
        for g in range(2):
            part = jnp.where(owner == g, queries, jnp.zeros_like(queries))
            streams.append(
                (
                    lambda i, part=part: jnp.dot(
                        keys[256 * i : 256 * i + 256], part, preferred_element_type=F32
                    ),
                    values_t[g * WIDE : (g + 1) * WIDE],
                    scores.at[g],
                    weights.at[g],
                    (),
                )
            )
    for n, (numer, m) in enumerate(attend_all(streams)):
        out = packed_result(numer, m).astype(BF)
        for i in range(4):
            out_ref[8 * (n % 2) + 4 * (n // 2) + i] = out[:, i * 128 : (i + 1) * 128]


def middle(scalars, received):
    return pl.pallas_call(
        middle_kernel,
        grid_spec=pltpu.PrefetchScalarGridSpec(
            num_scalar_prefetch=1,
            grid=(1,),
            in_specs=[pl.BlockSpec((16, 192, 128), lambda i, s: (0, 0, 0))],
            out_specs=pl.BlockSpec((16, WIDE, 128), lambda i, s: (0, 0, 0)),
            scratch_shapes=[pltpu.VMEM((128, 1024), BF)] * 3
            + [
                pltpu.VMEM((1024, 128), BF),
                pltpu.VMEM((2, 1024, 512), F32),
                pltpu.VMEM((2, 1024, 512), BF),
            ],
        ),
        out_shape=jax.ShapeDtypeStruct((16, WIDE, 128), BF),
        cost_estimate=pl.CostEstimate(
            flops=10_000_000_000, bytes_accessed=1_000_000, transcendentals=2_100_000
        ),
        name="middle",
    )(scalars, received)


def far_kernel(own_ref, *refs):
    key_refs = (own_ref,) + refs[:3]
    in_ref, mid_ref, out_ref, scores, weights, values_t = refs[3:]
    for c in range(8):
        block = key_refs[c // 2][16 * (c % 2) : 16 * (c % 2) + 16].reshape(512, 128)
        values_t[:, 512 * c : 512 * c + 512] = block.T[WIDE:]
    packed = in_ref[:, 32:48].reshape(256, 128).astype(F32)
    queries = jnp.concatenate([packed, pltpu.roll(packed, WIDE, 1)], axis=0)
    queries = jnp.where(lanes(queries.shape) < WIDE, queries, 0.0).astype(BF)

    def score(c):
        block = key_refs[c // 4][8 * (c % 4) : 8 * (c % 4) + 8]
        return nt(block.reshape(256, 128), queries)

    numer, m = attend(score, values_t[...], scores, weights, range(4))
    out = packed_result(numer, m)
    out = jnp.concatenate([out[:, :256], out[:, 256:]], axis=0).T.astype(BF)
    out_ref[:, :16] = out.reshape(16, 16, 128)
    out_ref[:, 16:] = mid_ref[:, :56]


def far(keys, received, mid_result):
    return pl.pallas_call(
        far_kernel,
        out_shape=jax.ShapeDtypeStruct((16, 72, 128), BF),
        scratch_shapes=[
            pltpu.VMEM((4096, 512), F32),
            pltpu.VMEM((4096, 512), BF),
            pltpu.VMEM((WIDE, 4096), BF),
        ],
        cost_estimate=pl.CostEstimate(
            flops=10_000_000_000, bytes_accessed=1_000_000, transcendentals=2_100_000
        ),
        name="far",
    )(*keys, received, mid_result)


def finish_kernel(
    s_ref, near0, near1, near2, in_ref, x_hbm, gain_ref, w_hbm, out_ref, mixed, x_ref, w_ref, near_ref, sems
):
    arrivals = {}
    for n, (source, first, heads) in enumerate(((near0, 0, 5), (near0, 5, 5), (near1, 10, 4), (near2, 14, 2))):
        part = source.at[5:10] if n == 1 else source.at[0:heads]
        arrivals[first] = pltpu.make_async_copy(part, near_ref.at[first : first + heads], sems.at[n])
        arrivals[first].start()
    copies = [
        pltpu.make_async_copy(x_hbm, x_ref, sems.at[4]),
        pltpu.make_async_copy(w_hbm, w_ref, sems.at[5]),
    ]
    for copy in copies:
        copy.start()
    lane = lanes((1, ROWS))
    column4 = lanes((128, ROWS)) - 4 * lax.broadcasted_iota(jnp.int32, (128, ROWS), 0)
    column16 = lanes((16, 256)) - 16 * lax.broadcasted_iota(jnp.int32, (16, 256), 0)
    for h in range(HEADS):
        off = s_ref[2 + h]
        off4 = off % 4
        off16 = off % 16
        if h in arrivals:
            arrivals[h].wait()
        mean_n, lse_n = to_lse(near_ref[h], near_ref[h, HEAD + 1 : HEAD + 2])
        spread4 = jnp.where(column4 == off4, 1.0, 0.0).astype(BF)
        mid = jnp.dot(
            in_ref[h, 16:], spread4, preferred_element_type=F32
        )
        spread16 = jnp.where(column16 == off16, 1.0, 0.0).astype(BF)
        distant = lax.dot_general(
            in_ref[h, :16], spread16, (((0,), (0,)), ((), ())), preferred_element_type=F32
        )
        distant = jnp.concatenate([distant[:WIDE], distant[WIDE:]], axis=1)

        def lse_of(spread):
            lse = spread[HEAD : HEAD + 1] + spread[HEAD + 1 : HEAD + 2]
            return lse + spread[HEAD + 2 : HEAD + 3]

        lse_m = jnp.where(lane % 4 == off4, lse_of(mid), NEGATIVE)
        lse_f = jnp.where(lane % 16 == off16, lse_of(distant), NEGATIVE)
        top = jnp.maximum(jnp.maximum(lse_n, lse_m), lse_f)
        weight_n = jnp.exp2(lse_n - top)
        weight_m = jnp.exp2(lse_m - top)
        weight_f = jnp.exp2(lse_f - top)
        inverse = 1.0 / jnp.maximum(weight_n + weight_m + weight_f, 1.0)
        mixed[HEAD * h : HEAD * (h + 1)] = (
            mean_n[:HEAD] * (weight_n * inverse)
            + mid[:HEAD] * (weight_m * inverse)
            + distant[:HEAD] * (weight_f * inverse)
        ).astype(BF)
    attended = mixed[...].T.astype(F32)
    sub = norm_rows(attended, gain_ref[...]).astype(BF)
    for copy in copies:
        copy.wait()
    out = x_ref[...].astype(F32) + jnp.dot(sub, w_ref[...], preferred_element_type=F32)
    out_ref[...] = out.astype(BF)


def finish(scalars, near_results, dilated, rows, gain, w_out):
    def whole(*shape):
        return pl.BlockSpec(shape, lambda i, s: (0,) * len(shape))

    return pl.pallas_call(
        finish_kernel,
        grid_spec=pltpu.PrefetchScalarGridSpec(
            num_scalar_prefetch=1,
            grid=(1,),
            in_specs=[
                pl.BlockSpec(memory_space=pl.ANY),
                pl.BlockSpec(memory_space=pl.ANY),
                pl.BlockSpec(memory_space=pl.ANY),
                whole(16, 72, 128),
                pl.BlockSpec(memory_space=pl.ANY),
                whole(1, WIDTH),
                pl.BlockSpec(memory_space=pl.ANY),
            ],
            out_specs=whole(ROWS, WIDTH),
            scratch_shapes=[
                pltpu.VMEM((WIDTH, ROWS), BF),
                pltpu.VMEM((ROWS, WIDTH), BF),
                pltpu.VMEM((WIDTH, WIDTH), BF),
                pltpu.VMEM((HEADS, WIDE, ROWS), F32),
                pltpu.SemaphoreType.DMA((6,)),
            ],
        ),
        out_shape=jax.ShapeDtypeStruct((ROWS, WIDTH), BF),
        name="finish",
    )(scalars, *near_results, dilated, rows, gain, w_out)


def exchange(value, axis):
    return lax.all_to_all(value, axis, split_axis=0, concat_axis=0, tiled=True)


def body(tile_embed, valid_tiles, offsets, norm_gain, w_qkv, sub_gain, w_out):
    position = lax.axis_index(("y", "xh", "xl", "z"))
    scalars = jnp.concatenate([valid_tiles, position.astype(jnp.int32)[None], offsets])
    gain, last_gain = norm_gain[None], sub_gain[None]
    arrived = exchange(tile_embed.reshape(128, 4, WIDTH), ("y", "xh", "xl", "z"))
    rows = arrived.transpose(1, 0, 2).reshape(ROWS, WIDTH)
    partner = lax.ppermute(rows, "z", [(i, i ^ 1) for i in range(8)])
    weights = widen(w_qkv)
    own, send = project(scalars, rows, gain, weights)
    received = exchange(send, ("xl", "z"))
    mine = received[:, :32]
    other = lax.ppermute(mine, "xh", [(0, 1), (1, 0)])
    keys = [jnp.concatenate([mine, other])]
    for y in range(1, 4):
        keys.append(lax.ppermute(keys[0], "y", [(i, (i + y) % 4) for i in range(4)]))
    near_results = []
    for first, count in ((0, 5), (5, 2), (7, 1)):
        near_results.append(near(scalars, partner, gain, weights, own, first, count))
    mid_result = middle(scalars, received)
    far_result = far(keys, received, mid_result)
    dilated = exchange(far_result, ("xl", "z"))
    return finish(scalars, near_results, dilated, rows, last_gain, w_out)


def solution(mesh):
    inner = Mesh(mesh.devices.reshape(4, 2, 2, 8, 2), ("y", "xh", "xl", "z", "slide"))
    split = P(("slide", "y", "xh", "xl", "z"), None)
    return jax.shard_map(
        body,
        mesh=inner,
        in_specs=(split, P("slide"), P(), P(), P(), P(), P()),
        out_specs=split,
        check_vma=False,
    )
```

```python
import math

import jax
import jax.numpy as jnp
from jax import lax
from jax.experimental import pallas as pl
from jax.experimental.pallas import tpu as pltpu
from jax.sharding import Mesh, PartitionSpec as P


HEADS = 16
HEAD = 48
WIDE = 64
ROWS = 512
WIDTH = 768
NEGATIVE = -1e30
EPSILON = 1e-05
SCALE = math.log2(math.e) / math.sqrt(HEAD)
BF = jnp.bfloat16
F32 = jnp.float32


def norm_rows(x, gain):
    mean = jnp.mean(x, axis=-1, keepdims=True)
    centred = x - mean
    var = jnp.mean(centred * centred, axis=-1, keepdims=True)
    return centred * lax.rsqrt(var + EPSILON) * gain


def lanes(shape):
    return lax.broadcasted_iota(jnp.int32, shape, len(shape) - 1)


def mask_key_value(k, v, first, valid):
    lane = lanes(k.shape)
    special = lane % WIDE == HEAD
    alive = first + lax.broadcasted_iota(jnp.int32, k.shape, 0) < valid
    k = jnp.where(special, jnp.where(alive, 0.0, NEGATIVE), k)
    v = jnp.where(alive, jnp.where(special, 1.0, v), 0.0)
    return k, v


def nt(a, b):
    return lax.dot_general(a, b, (((1,), (1,)), ((), ())), preferred_element_type=F32)


def widen_kernel(w_ref, out_ref):
    for j, start in enumerate((WIDTH, 2 * WIDTH, 0)):
        for p in range(8):
            first = start + 2 * HEAD * p
            window = first // 128 * 128
            row = lax.broadcasted_iota(jnp.int32, (256, 128), 0) + (window - first)
            lane = lanes((256, 128))
            column = lane % WIDE + lane // WIDE * HEAD
            chosen = (row == column) & (lane % WIDE < HEAD)
            pick = jnp.where(chosen, 1.0, 0.0).astype(BF)
            wide = min(256, 3 * WIDTH - window)
            part = jnp.dot(
                w_ref[:, window : window + wide], pick[:wide], preferred_element_type=F32
            )
            column = 512 + 128 * (p % 2) if j == 2 else 256 * (p % 2) + 128 * j
            out_ref[p // 2, :, column : column + 128] = part.astype(BF)


def widen(w_qkv):
    return pl.pallas_call(
        widen_kernel,
        out_shape=jax.ShapeDtypeStruct((4, WIDTH, WIDTH), BF),
        cost_estimate=pl.CostEstimate(
            flops=10_000_000_000, bytes_accessed=8_000_000, transcendentals=0
        ),
        name="widen",
    )(w_qkv)


def project_kernel(s_ref, x_ref, gain_ref, w_ref, own_ref, send_ref, normed, stage):
    p = pl.program_id(0)

    @pl.when(p == 0)
    def _():
        normed[...] = norm_rows(x_ref[...].astype(F32), gain_ref[...]).astype(BF)

    rows = normed[...]
    projected = jnp.dot(rows, w_ref[0], preferred_element_type=F32)
    projected = projected.astype(BF).astype(F32)
    for u in range(2):
        k = projected[:, 256 * u : 256 * u + 128]
        v = projected[:, 256 * u + 128 : 256 * u + 256]
        q = projected[:, 512 + 128 * u : 640 + 128 * u]
        k, v = mask_key_value(k, v, s_ref[1] * ROWS, s_ref[0])
        q = jnp.where(lanes(q.shape) % WIDE == HEAD, 1.0, q)
        stage[u, 0] = k
        stage[u, 1] = v
        stage[u, 2] = q
        own_ref[u, 0] = k.astype(BF)
        own_ref[u, 1] = v.astype(BF)
        own_ref[u, 2] = q.astype(BF)
        low = lanes((ROWS // 4, 128)) < WIDE
        off = [s_ref[2 + 4 * p + 2 * u + a] for a in range(2)]
        for j in range(3):
            first = stage[u, j, pl.ds(off[0] % 4, ROWS // 4, stride=4), :]
            second = stage[u, j, pl.ds(off[1] % 4, ROWS // 4, stride=4), :]
            chosen = jnp.where(low, first, second).astype(BF).T
            for a in range(2):
                send_ref[2 * u + a, HEAD * (j + 1) : HEAD * (j + 2)] = chosen[a * WIDE : a * WIDE + HEAD]
        low = lanes((ROWS // 16, 128)) < WIDE
        for a in range(2):
            k, v, q = [stage[u, j, pl.ds(off[a] % 16, ROWS // 16, stride=16), :] for j in range(3)]
            if a == 0:
                v = pltpu.roll(v, WIDE, 1)
                q_high = pltpu.roll(q, WIDE, 1)
            else:
                k = pltpu.roll(k, WIDE, 1)
                q_high = q
                q = pltpu.roll(q, WIDE, 1)
            send_ref[2 * u + a, :32] = jnp.where(low, k, v).astype(BF)
            send_ref[2 * u + a, 32:48] = jnp.where(low[:16], q[:16], q_high[16:]).astype(BF)


def project(scalars, rows, gain, weights):
    return pl.pallas_call(
        project_kernel,
        grid_spec=pltpu.PrefetchScalarGridSpec(
            num_scalar_prefetch=1,
            grid=(4,),
            in_specs=[
                pl.BlockSpec((ROWS, WIDTH), lambda p, s: (0, 0)),
                pl.BlockSpec((1, WIDTH), lambda p, s: (0, 0)),
                pl.BlockSpec((1, WIDTH, WIDTH), lambda p, s: (p, 0, 0)),
            ],
            out_specs=[
                pl.BlockSpec((2, 3, ROWS, 128), lambda p, s: (p, 0, 0, 0)),
                pl.BlockSpec((4, 192, 128), lambda p, s: (p, 0, 0)),
            ],
            scratch_shapes=[pltpu.VMEM((ROWS, WIDTH), BF), pltpu.VMEM((2, 3, ROWS, 128), F32)],
        ),
        out_shape=[
            jax.ShapeDtypeStruct((8, 3, ROWS, 128), BF),
            jax.ShapeDtypeStruct((16, 192, 128), BF),
        ],
        name="project",
    )(scalars, rows, gain, weights)


def attend_all(streams):
    results = []
    tops = [None] * len(streams)

    def score_block(n, c):
        score, _, scores, _, _ = streams[n]
        s = score(c) * SCALE
        scores[256 * c : 256 * c + 256] = s
        part = jnp.max(s.reshape(32, 8, s.shape[1]), axis=0)
        tops[n] = part if tops[n] is None else jnp.maximum(tops[n], part)

    for c in range(streams[0][2].shape[0] // 256):
        score_block(0, c)
    for n, (_, values_t, scores, weights, bonus) in enumerate(streams):
        m = jnp.max(tops[n], axis=0, keepdims=True)
        for c in range(scores.shape[0] // 256):
            if n + 1 < len(streams):
                score_block(n + 1, c)
            shift = m - (1.0 if c in bonus else 0.0)
            block = slice(256 * c, 256 * c + 256)
            weights[block] = jnp.exp2(scores[block] - shift).astype(BF)
        results.append((jnp.dot(values_t, weights[...], preferred_element_type=F32), m))
    return results


def near_kernel(s_ref, x_ref, gain_ref, w_ref, own_ref, out_ref, normed, keys, scores, weights):
    p = pl.program_id(0)

    @pl.when(p == 0)
    def _():
        normed[...] = norm_rows(x_ref[...].astype(F32), gain_ref[...]).astype(BF)

    rows = normed[...]
    projected = jnp.dot(rows, w_ref[0], preferred_element_type=F32).astype(BF).astype(F32)
    k, v = projected[:, :128], projected[:, 128:]
    partner = s_ref[1] + 1 - 2 * (s_ref[1] % 2)
    k, v = mask_key_value(k, v, partner * ROWS, s_ref[0])
    keys[:ROWS] = own_ref[0, 0]
    keys[ROWS:] = k.astype(BF)
    values_t = jnp.concatenate([own_ref[0, 1], v.astype(BF)], axis=0).T
    queries = own_ref[0, 2]
    streams = []
    for a in range(2):
        part = jnp.where(lanes(queries.shape) // WIDE == a, queries, jnp.zeros_like(queries))
        streams.append(
            (
                lambda i, part=part: nt(keys[256 * i : 256 * i + 256], part),
                values_t[a * WIDE : (a + 1) * WIDE],
                scores.at[a],
                weights.at[a],
                (),
            )
        )
    for a, (numer, m) in enumerate(attend_all(streams)):
        row = lax.broadcasted_iota(jnp.int32, numer.shape, 0)
        out_ref[a] = jnp.where(row == HEAD + 1, m, numer)


def near(scalars, rows, gain, weights, own, first, count):
    return pl.pallas_call(
        near_kernel,
        grid_spec=pltpu.PrefetchScalarGridSpec(
            num_scalar_prefetch=1,
            grid=(count,),
            in_specs=[
                pl.BlockSpec((ROWS, WIDTH), lambda p, s: (0, 0)),
                pl.BlockSpec((1, WIDTH), lambda p, s: (0, 0)),
                pl.BlockSpec(
                    (1, WIDTH, 256), lambda p, s: ((p + first) // 2, 0, (p + first) % 2)
                ),
                pl.BlockSpec((1, 3, ROWS, 128), lambda p, s: (p + first, 0, 0, 0)),
            ],
            out_specs=pl.BlockSpec((2, WIDE, ROWS), lambda p, s: (p, 0, 0)),
            scratch_shapes=[
                pltpu.VMEM((ROWS, WIDTH), BF),
                pltpu.VMEM((2 * ROWS, 128), BF),
                pltpu.VMEM((2, 2 * ROWS, ROWS), F32),
                pltpu.VMEM((2, 2 * ROWS, ROWS), BF),
            ],
        ),
        out_shape=jax.ShapeDtypeStruct((2 * count, WIDE, ROWS), F32),
        cost_estimate=pl.CostEstimate(
            flops=5_000_000_000 * count,
            bytes_accessed=1_000_000 * count,
            transcendentals=1_050_000 * count,
        ),
        name="near",
    )(scalars, rows, gain, weights, own)


def to_lse(numer, m):
    total = numer[HEAD : HEAD + 1]
    lse = jnp.where(total > 0.0, m + jnp.log2(jnp.maximum(total, 1.0)), NEGATIVE)
    return numer / jnp.maximum(total, 1.0), lse


def packed_result(numer, m):
    mean, lse = to_lse(numer, m)
    high = lse.astype(BF).astype(F32)
    rest = lse - high
    second = rest.astype(BF).astype(F32)
    third = rest - second
    row = lax.broadcasted_iota(jnp.int32, mean.shape, 0)
    out = jnp.where(row < HEAD, mean, 0.0)
    out = jnp.where(row == HEAD, high, out)
    out = jnp.where(row == HEAD + 1, second, out)
    return jnp.where(row == HEAD + 2, third, out)


def middle_kernel(s_ref, in_ref, out_ref, keys_t, values_t, queries_t, keys, scores, weights):
    off4 = s_ref[2 + s_ref[1] % HEADS] % 4
    row = lax.broadcasted_iota(jnp.int32, (WIDE - HEAD, 1024), 0)
    first = row == 0
    for g in range(2):
        base = g * WIDE
        for i in range(8):
            part = slice(i * 128, (i + 1) * 128)
            for j, ref in enumerate((keys_t, values_t, queries_t)):
                ref[base : base + HEAD, part] = in_ref[8 * g + i, HEAD * (j + 1) : HEAD * (j + 2)]
        start = (s_ref[1] // HEADS * 2 + g) * 4096 + off4
        alive = start + 4 * lanes(row.shape) < s_ref[0]
        spare = slice(base + HEAD, base + WIDE)
        keys_t[spare] = jnp.where(first & (~alive), NEGATIVE, 0.0).astype(BF)
        values_t[spare] = jnp.where(first & alive, 1.0, 0.0).astype(BF)
        queries_t[spare] = jnp.where(first, 1.0, 0.0).astype(BF)
        alive = start + 4 * lanes((HEAD, 1024)) < s_ref[0]
        values = values_t[base : base + HEAD]
        values_t[base : base + HEAD] = jnp.where(alive, values, jnp.zeros_like(values))
    keys[...] = keys_t[...].T
    streams = []
    for c in range(0, 1024, 512):
        queries = queries_t[:, c : c + 512]
        owner = lax.broadcasted_iota(jnp.int32, queries.shape, 0) // WIDE
        for g in range(2):
            part = jnp.where(owner == g, queries, jnp.zeros_like(queries))
            streams.append(
                (
                    lambda i, part=part: jnp.dot(
                        keys[256 * i : 256 * i + 256], part, preferred_element_type=F32
                    ),
                    values_t[g * WIDE : (g + 1) * WIDE],
                    scores.at[g],
                    weights.at[g],
                    (),
                )
            )
    for n, (numer, m) in enumerate(attend_all(streams)):
        out = packed_result(numer, m).astype(BF)
        for i in range(4):
            out_ref[8 * (n % 2) + 4 * (n // 2) + i] = out[:, i * 128 : (i + 1) * 128]


def middle(scalars, received):
    return pl.pallas_call(
        middle_kernel,
        grid_spec=pltpu.PrefetchScalarGridSpec(
            num_scalar_prefetch=1,
            grid=(1,),
            in_specs=[pl.BlockSpec((16, 192, 128), lambda i, s: (0, 0, 0))],
            out_specs=pl.BlockSpec((16, WIDE, 128), lambda i, s: (0, 0, 0)),
            scratch_shapes=[pltpu.VMEM((128, 1024), BF)] * 3
            + [
                pltpu.VMEM((1024, 128), BF),
                pltpu.VMEM((2, 1024, 512), F32),
                pltpu.VMEM((2, 1024, 512), BF),
            ],
        ),
        out_shape=jax.ShapeDtypeStruct((16, WIDE, 128), BF),
        cost_estimate=pl.CostEstimate(
            flops=10_000_000_000, bytes_accessed=1_000_000, transcendentals=2_100_000
        ),
        name="middle",
    )(scalars, received)


def far_kernel(own_ref, *refs):
    key_refs = (own_ref,) + refs[:3]
    in_ref, mid_ref, out_ref, scores, weights, values_t = refs[3:]
    for c in range(8):
        block = key_refs[c // 2][16 * (c % 2) : 16 * (c % 2) + 16].reshape(512, 128)
        values_t[:, 512 * c : 512 * c + 512] = block.T[WIDE:]
    packed = in_ref[:, 32:48].reshape(256, 128).astype(F32)
    queries = jnp.concatenate([packed, pltpu.roll(packed, WIDE, 1)], axis=0)
    queries = jnp.where(lanes(queries.shape) < WIDE, queries, 0.0).astype(BF)

    streams = []
    for half in range(2):
        part = queries[256 * half : 256 * half + 256]

        def score(c, part=part):
            block = key_refs[c // 4][8 * (c % 4) : 8 * (c % 4) + 8]
            return nt(block.reshape(256, 128), part)

        streams.append((score, values_t[...], scores.at[half], weights.at[half], range(4)))
    out = [packed_result(numer, m) for numer, m in attend_all(streams)]
    out = jnp.concatenate(out, axis=0).T.astype(BF)
    out_ref[:, :16] = out.reshape(16, 16, 128)
    out_ref[:, 16:] = mid_ref[:, :56]


def far(keys, received, mid_result):
    return pl.pallas_call(
        far_kernel,
        out_shape=jax.ShapeDtypeStruct((16, 72, 128), BF),
        scratch_shapes=[
            pltpu.VMEM((2, 4096, 256), F32),
            pltpu.VMEM((2, 4096, 256), BF),
            pltpu.VMEM((WIDE, 4096), BF),
        ],
        cost_estimate=pl.CostEstimate(
            flops=10_000_000_000, bytes_accessed=1_000_000, transcendentals=2_100_000
        ),
        name="far",
    )(*keys, received, mid_result)


def finish_kernel(s_ref, near0_ref, near1_ref, near2_ref, in_ref, x_ref, gain_ref, w_ref, out_ref, mixed):
    lane = lanes((1, ROWS))
    column4 = lanes((128, ROWS)) - 4 * lax.broadcasted_iota(jnp.int32, (128, ROWS), 0)
    column16 = lanes((16, 256)) - 16 * lax.broadcasted_iota(jnp.int32, (16, 256), 0)
    for h in range(HEADS):
        off = s_ref[2 + h]
        off4 = off % 4
        off16 = off % 16
        near_ref = near0_ref if h < 10 else near1_ref if h < 14 else near2_ref
        i = h if h < 10 else h - 10 if h < 14 else h - 14
        mean_n, lse_n = to_lse(near_ref[i], near_ref[i, HEAD + 1 : HEAD + 2])
        spread4 = jnp.where(column4 == off4, 1.0, 0.0).astype(BF)
        mid = jnp.dot(
            in_ref[h, 16:], spread4, preferred_element_type=F32
        )
        spread16 = jnp.where(column16 == off16, 1.0, 0.0).astype(BF)
        distant = lax.dot_general(
            in_ref[h, :16], spread16, (((0,), (0,)), ((), ())), preferred_element_type=F32
        )
        distant = jnp.concatenate([distant[:WIDE], distant[WIDE:]], axis=1)

        def lse_of(spread):
            lse = spread[HEAD : HEAD + 1] + spread[HEAD + 1 : HEAD + 2]
            return lse + spread[HEAD + 2 : HEAD + 3]

        lse_m = jnp.where(lane % 4 == off4, lse_of(mid), NEGATIVE)
        lse_f = jnp.where(lane % 16 == off16, lse_of(distant), NEGATIVE)
        top = jnp.maximum(jnp.maximum(lse_n, lse_m), lse_f)
        weight_n = jnp.exp2(lse_n - top)
        weight_m = jnp.exp2(lse_m - top)
        weight_f = jnp.exp2(lse_f - top)
        inverse = 1.0 / jnp.maximum(weight_n + weight_m + weight_f, 1.0)
        mixed[HEAD * h : HEAD * (h + 1)] = (
            mean_n[:HEAD] * (weight_n * inverse)
            + mid[:HEAD] * (weight_m * inverse)
            + distant[:HEAD] * (weight_f * inverse)
        ).astype(BF)
    attended = mixed[...].T.astype(F32)
    sub = norm_rows(attended, gain_ref[...]).astype(BF)
    out = x_ref[...].astype(F32) + jnp.dot(sub, w_ref[...], preferred_element_type=F32)
    out_ref[...] = out.astype(BF)


def finish(scalars, near_results, dilated, rows, gain, w_out):
    def whole(*shape):
        return pl.BlockSpec(shape, lambda i, s: (0,) * len(shape))

    return pl.pallas_call(
        finish_kernel,
        grid_spec=pltpu.PrefetchScalarGridSpec(
            num_scalar_prefetch=1,
            grid=(1,),
            in_specs=[
                whole(10, WIDE, ROWS),
                whole(4, WIDE, ROWS),
                whole(2, WIDE, ROWS),
                whole(16, 72, 128),
                whole(ROWS, WIDTH),
                whole(1, WIDTH),
                whole(WIDTH, WIDTH),
            ],
            out_specs=whole(ROWS, WIDTH),
            scratch_shapes=[pltpu.VMEM((WIDTH, ROWS), BF)],
        ),
        out_shape=jax.ShapeDtypeStruct((ROWS, WIDTH), BF),
        name="finish",
    )(scalars, *near_results, dilated, rows, gain, w_out)


def exchange(value, axis):
    return lax.all_to_all(value, axis, split_axis=0, concat_axis=0, tiled=True)


def body(tile_embed, valid_tiles, offsets, norm_gain, w_qkv, sub_gain, w_out):
    position = lax.axis_index(("y", "xh", "xl", "z"))
    scalars = jnp.concatenate([valid_tiles, position.astype(jnp.int32)[None], offsets])
    gain, last_gain = norm_gain[None], sub_gain[None]
    arrived = exchange(tile_embed.reshape(128, 4, WIDTH), ("y", "xh", "xl", "z"))
    rows = arrived.transpose(1, 0, 2).reshape(ROWS, WIDTH)
    partner = lax.ppermute(rows, "z", [(i, i ^ 1) for i in range(8)])
    weights = widen(w_qkv)
    own, send = project(scalars, rows, gain, weights)
    received = exchange(send, ("xl", "z"))
    mine = received[:, :32]
    other = lax.ppermute(mine, "xh", [(0, 1), (1, 0)])
    keys = [jnp.concatenate([mine, other])]
    for y in range(1, 4):
        keys.append(lax.ppermute(keys[0], "y", [(i, (i + y) % 4) for i in range(4)]))
    near_results = []
    for first, count in ((0, 5), (5, 2), (7, 1)):
        near_results.append(near(scalars, partner, gain, weights, own, first, count))
    mid_result = middle(scalars, received)
    far_result = far(keys, received, mid_result)
    dilated = exchange(far_result, ("xl", "z"))
    return finish(scalars, near_results, dilated, rows, last_gain, w_out)


def solution(mesh):
    inner = Mesh(mesh.devices.reshape(4, 2, 2, 8, 2), ("y", "xh", "xl", "z", "slide"))
    split = P(("slide", "y", "xh", "xl", "z"), None)
    return jax.shard_map(
        body,
        mesh=inner,
        in_specs=(split, P("slide"), P(), P(), P(), P(), P()),
        out_specs=split,
        check_vma=False,
    )
```
